32 devices in a mesh: dp: 1 (over z), ep: 32 (over y, x, core).
Axes of the slice: x: 4, y: 4, z: 1, core: 2. Of those that a mesh axis runs over, the one named last changes fastest.
The devices are a block of a 4x4x8 slice.
Arguments:
- hidden: bfloat16 [8192, 2048], P(('dp', 'ep'))
- router_w: float32 [2048, 32], replicated
- expert_ids: int32 [8192, 2], P(('dp', 'ep'))
- w_gate: bfloat16 [32, 2048, 2048], P('ep')
- w_up: bfloat16 [32, 2048, 2048], P('ep')
- w_down: bfloat16 [32, 2048, 2048], P('ep')
- post_scale: float32 [2], replicated
Outputs:
- output: bfloat16 [8192, 2048], P(('dp', 'ep'))
All inputs are finite; a program needn't handle non-finite values.
Results may differ from the reference program's by a relative error of at most 0.001.
Values are sent between devices in bfloat16 or wider.
A program may use at most 768 MiB of HBM per device.

```python
import jax
import jax.numpy as jnp
from jax import lax

GROUP_SIZE = 32
TOKENS_DEV = 256
EXPERTS = 32
HIDDEN = 2048
FFN_DIM = 2048
TOP_K = 2
BATCH_ROWS = GROUP_SIZE * TOKENS_DEV
HOT_COUNT = max(1, EXPERTS // 8)
CAPACITY = TOKENS_DEV // HOT_COUNT
MAX_ROWS = GROUP_SIZE * CAPACITY


def draw_routing(ids_key, part):
    order_key, shard_key = jax.random.split(ids_key)
    expert_order = jax.random.permutation(order_key, EXPERTS)
    hot_ids = expert_order[:HOT_COUNT]
    cold_ids = expert_order[HOT_COUNT:]
    shard_keys = jax.random.split(jax.random.fold_in(shard_key, part), GROUP_SIZE)

    def one_shard(one_key):
        tok_key, cold_key, swap_key = jax.random.split(one_key, 3)
        tok_rank = jax.random.permutation(tok_key, TOKENS_DEV)
        cold_mix = jax.random.permutation(cold_key, cold_ids)
        first_pick = hot_ids[tok_rank % HOT_COUNT]
        second_pick = cold_mix[tok_rank % (EXPERTS - HOT_COUNT)]
        swapped = jax.random.randint(swap_key, (TOKENS_DEV,), 0, 2) == 1
        return jnp.stack([jnp.where(swapped, second_pick, first_pick), jnp.where(swapped, first_pick, second_pick)], axis=1)

    return jax.vmap(one_shard)(shard_keys).reshape(BATCH_ROWS, TOP_K).astype(jnp.int32)


def draw_experts(weight_key, row_count, col_count):
    expert_keys = jax.random.split(weight_key, EXPERTS)
    return lax.map(lambda one_key: (jax.random.normal(one_key, (row_count, col_count), jnp.float32) * row_count ** -0.5).astype(jnp.bfloat16), expert_keys)


def setup_inputs(seed: int = 0, part: int = 0) -> dict:
    base_key = jax.random.key(seed)
    hid_key, route_key, gate_key, up_key, down_key, post_key, ids_key = jax.random.split(base_key, 7)
    hidden = jax.random.normal(jax.random.fold_in(hid_key, part), (BATCH_ROWS, HIDDEN), jnp.float32).astype(jnp.bfloat16)
    router_w = jax.random.normal(route_key, (HIDDEN, EXPERTS), jnp.float32) * (0.4 * HIDDEN ** -0.5)
    w_gate = draw_experts(gate_key, HIDDEN, FFN_DIM)
    w_up = draw_experts(up_key, HIDDEN, FFN_DIM)
    w_down = draw_experts(down_key, FFN_DIM, HIDDEN)
    post_scale = jax.random.uniform(post_key, (2,), jnp.float32, jnp.array([0.5, 1.0], jnp.float32), jnp.array([1.0, 2.0], jnp.float32))
    expert_ids = draw_routing(ids_key, part)
    return {'hidden': hidden, 'router_w': router_w, 'expert_ids': expert_ids, 'w_gate': w_gate, 'w_up': w_up, 'w_down': w_down, 'post_scale': post_scale}


def reference(hidden, router_w, expert_ids, w_gate, w_up, w_down, post_scale):
    hid_wide = hidden.astype(jnp.float32)
    logits = jnp.dot(hid_wide, router_w, preferred_element_type=jnp.float32)
    router_prob = jax.nn.softmax(logits, axis=-1)
    picked = jnp.take_along_axis(router_prob, expert_ids, axis=1)
    gates = picked / jnp.sum(picked, axis=1, keepdims=True)

    def add_expert(running_sum, expert):
        hit_mask = expert_ids == expert
        tok_gate = jnp.sum(jnp.where(hit_mask, gates, 0.0), axis=1)
        chosen = jnp.any(hit_mask, axis=1)
        row_index = jnp.nonzero(chosen, size=MAX_ROWS, fill_value=0)[0]
        in_range = jnp.arange(MAX_ROWS) < jnp.sum(chosen)
        tok_rows = hidden[row_index]
        gate_in = jnp.dot(tok_rows, w_gate[expert], preferred_element_type=jnp.float32)
        up_in = jnp.dot(tok_rows, w_up[expert], preferred_element_type=jnp.float32)
        middle = (jax.nn.silu(gate_in) * up_in).astype(jnp.bfloat16)
        expert_out = jnp.dot(middle, w_down[expert], preferred_element_type=jnp.float32).astype(jnp.bfloat16)
        row_weight = jnp.where(in_range, tok_gate[row_index], 0.0)
        running_sum = running_sum.at[row_index].add(row_weight[:, None] * expert_out.astype(jnp.float32))
        return running_sum, None

    mixed, _ = lax.scan(add_expert, jnp.zeros((BATCH_ROWS, HIDDEN), jnp.float32), jnp.arange(EXPERTS))
    return (post_scale[0] * hid_wide + post_scale[1] * mixed).astype(jnp.bfloat16)
```

```python
import functools
import jax
import jax.numpy as jnp
from jax import lax
from jax.experimental import pallas as pl
from jax.experimental.pallas import tpu as pltpu
from jax.sharding import PartitionSpec as P

MESH = pl.DeviceIdType.MESH
SIDE = 4

CODE = 0
GATHER = 3
CHUNK = 9
LEG = 17
BACK = 19
BLEG = 27
HOME = 29
HLEG = 61
NMSG = 69
SFWD = 69
SBFWD = 71
SLEG2 = 73
SHFWD = 74
SNBR = 82
SBACK = 86
SHOME = 93
NSEND = 117


def kernel_body(hid, code, code_col, gates, scale, w1h, w3h, w2h,
                out, fwd, back, bleg, hleg,
                w1, w3, w2, got, codes, pbuf, xs, outq, mid, ret, acc,
                send, recv, wsem, lsem):
    tokens, width = hid.shape
    cap = xs.shape[1] // SIDE
    ffn = w1.shape[1]
    half = tokens // 2
    tile = min(512, width)
    me = lax.axis_index('ep')
    y, x, c = lax.div(me, 2 * SIDE), lax.rem(lax.div(me, 2), SIDE), lax.rem(me, 2)

    def dev(yy, xx, cc):
        return (lax.rem(yy, SIDE) * SIDE + lax.rem(xx, SIDE)) * 2 + cc

    def qdev(o, core, axis):
        return dev(y + (1 - axis) * o, x + axis * o, core)

    def pdev(o):
        return dev(y + c * o, x + (1 - c) * o, c)

    def rcopy(src, dst, sid, rid, to):
        return pltpu.make_async_remote_copy(src_ref=src, dst_ref=dst, send_sem=send.at[sid], recv_sem=recv.at[rid], device_id={'ep': to}, device_id_type=MESH)

    sent = []

    def put(src, dst, sid, rid, to):
        cp = rcopy(src, dst, sid, rid, to)
        cp.start()
        sent.append((src, sid))

    def got_it(dst, rid):
        rcopy(dst, dst, 0, rid, me).wait_recv()

    lo, hi = pl.ds(0, half), pl.ds(half, half)

    for s, o in ((1, 1), (3, 3), (2, 2)):
        put(code, codes.at[s - 1], CODE + s - 1, CODE + s - 1, pdev(o))
    put(hid.at[lo], got.at[0, lo], GATHER + 0, GATHER + 0, pdev(1))
    put(hid.at[hi], got.at[2, hi], GATHER + 2, GATHER + 2, pdev(3))
    put(hid.at[hi], got.at[0, hi], GATHER + 1, GATHER + 1, pdev(1))
    put(hid.at[lo], got.at[2, lo], GATHER + 3, GATHER + 3, pdev(3))
    loads = [pltpu.make_async_copy(a, b, wsem.at[i]) for i, (a, b) in enumerate(((w1h, w1), (w3h, w3), (w2h, w2)))]
    for cp in loads:
        cp.start()

    order = (2, 1, 3, 0)

    def pack(s):
        cref = code if s == 0 else codes.at[s - 1]
        gref = hid if s == 0 else got.at[s - 1]
        c0, c1 = cref[0:1, :], cref[1:2, :]
        for i, o in enumerate(order):
            chip = lax.div(qdev(o, 0, c), 2)
            rows = lax.broadcasted_iota(jnp.int32, (2 * cap, tokens), 0) + chip * (2 * cap)
            hot = (rows == c0) | (rows == c1)
            pbuf[i * 2 * cap:(i + 1) * 2 * cap, :] = jnp.where(hot, 1.0, 0.0).astype(jnp.bfloat16)

        def one(t, carry):
            cols = pl.ds(pl.multiple_of(t * tile, tile), tile)
            r = jnp.dot(pbuf[...], gref[:, cols], preferred_element_type=jnp.float32).astype(jnp.bfloat16)
            dst = pl.ds(s * cap, cap)
            for i in range(6):
                outq[i, dst, cols] = r[i * cap:(i + 1) * cap]
            r0, r1 = r[6 * cap:7 * cap], r[7 * cap:8 * cap]
            own0 = c == 0
            xs[0, dst, cols] = jnp.where(own0, r0, r1)
            outq[6, dst, cols] = jnp.where(own0, r1, r0)
            return carry

        lax.fori_loop(0, width // tile, one, 0)

    pack(0)
    got_it(got.at[0, lo], GATHER + 0)
    put(got.at[0, lo], got.at[1, lo], GATHER + 4, GATHER + 4, pdev(1))
    got_it(got.at[2, hi], GATHER + 2)
    put(got.at[2, hi], got.at[1, hi], GATHER + 5, GATHER + 5, pdev(3))
    got_it(codes.at[0], CODE + 0)
    got_it(got.at[0, hi], GATHER + 1)
    pack(1)
    got_it(codes.at[2], CODE + 2)
    got_it(got.at[2, lo], GATHER + 3)
    pack(3)
    got_it(codes.at[1], CODE + 1)
    got_it(got.at[1, lo], GATHER + 4)
    got_it(got.at[1, hi], GATHER + 5)
    pack(2)

    put(outq.at[0], fwd.at[0], LEG + 0, LEG + 0, qdev(1, c, c))
    put(outq.at[1], fwd.at[1], LEG + 1, LEG + 1, qdev(3, c, c))
    put(outq.at[2], xs.at[2 + c], SNBR + 0, CHUNK + 2 + c, qdev(1, 0, c))
    put(outq.at[5], xs.at[2 + c], SNBR + 1, CHUNK + 2 + c, qdev(3, 1, c))
    put(outq.at[6], xs.at[1], CHUNK + 1, CHUNK + 1, qdev(0, 1 - c, c))
    put(outq.at[3], xs.at[6 + c], SNBR + 2, CHUNK + 6 + c, qdev(1, 1, c))
    put(outq.at[4], xs.at[6 + c], SNBR + 3, CHUNK + 6 + c, qdev(3, 0, c))

    def chunk_forward():
        got_it(fwd.at[0], LEG + 0)
        put(fwd.at[0], xs.at[4 + c], SFWD + 0, CHUNK + 4 + c, qdev(1, 0, c))
        got_it(fwd.at[1], LEG + 1)
        put(fwd.at[1], xs.at[4 + c], SFWD + 1, CHUNK + 4 + c, qdev(3, 1, c))

    locals_ = []

    def part(s):
        return pl.ds(s * cap, cap)

    def home(ref, blk, k, n):
        put(ref.at[part(1)], ret.at[8 + blk], SHOME + 3 * n, HOME + 8 + blk, pdev(3))
        put(ref.at[part(3)], ret.at[24 + blk], SHOME + 3 * n + 1, HOME + 24 + blk, pdev(1))
        put(ref.at[part(2)], hleg.at[blk], SHOME + 3 * n + 2, HLEG + blk, pdev(1 + 2 * k))

    def home_from(blk, k, n):
        got_it(back.at[blk], BACK + blk)
        home(back.at[blk], blk, k, n)
        cp = pltpu.make_async_copy(back.at[blk, part(0)], ret.at[blk], lsem.at[n])
        cp.start()
        locals_.append((blk, n))

    def home_forward(blk, n):
        got_it(hleg.at[blk], HLEG + blk)
        put(hleg.at[blk], ret.at[16 + blk], SHFWD + n, HOME + 16 + blk, pdev(1 + 2 * (blk % 2)))

    def back_forward():
        got_it(bleg.at[0], BLEG + 0)
        put(bleg.at[0], back.at[4], SBFWD + 0, BACK + 4, qdev(1, c, c))
        got_it(bleg.at[1], BLEG + 1)
        put(bleg.at[1], back.at[5], SBFWD + 1, BACK + 5, qdev(3, c, c))

    def after(step):
        if step == 0:
            ret[c] = xs[0, part(0), :]
            home(xs.at[0], c, c, 0)
        elif step == 1:
            put(xs.at[1], back.at[c], SBACK + 0, BACK + c, qdev(0, 1 - c, c))
            chunk_forward()
        elif step in (2, 3):
            put(xs.at[step], back.at[2 + 5 * c], SBACK + step - 1, BACK + 2 + 5 * c, qdev(3 + 2 * c, step % 2, step % 2))
            if step == 3:
                home_from(1 - c, 1 - c, 1)
        elif step in (4, 5):
            put(xs.at[step], bleg.at[c], SBACK + step - 1, BLEG + c, qdev(1 + 2 * c, step % 2, step % 2))
            if step == 5:
                for k in range(2):
                    home_forward(k, k)
        else:
            put(xs.at[step], back.at[6 - 3 * c], SBACK + step - 1, BACK + 6 - 3 * c, qdev(1 + 2 * c, step % 2, step % 2))

    for cp in loads:
        cp.wait()

    def expert(step):
        def up(t, carry):
            cols = pl.ds(pl.multiple_of(t * ftile, ftile), ftile)
            a = jnp.dot(xs[step], w1[:, cols], preferred_element_type=jnp.float32)
            b = jnp.dot(xs[step], w3[:, cols], preferred_element_type=jnp.float32)
            mid[:, cols] = (jax.nn.silu(a) * b).astype(jnp.bfloat16)
            return carry

        def down(t, carry):
            cols = pl.ds(pl.multiple_of(t * tile, tile), tile)
            xs[step, :, cols] = jnp.dot(mid[...], w2[:, cols], preferred_element_type=jnp.float32).astype(jnp.bfloat16)
            return carry

        ftile = min(512, ffn)
        lax.fori_loop(0, ffn // ftile, up, 0)
        lax.fori_loop(0, width // tile, down, 0)

    def step_body(step, carry):
        @pl.when(step > 0)
        def _():
            got_it(xs.at[step], CHUNK + step)
        expert(step)
        for j in range(8):
            @pl.when(step == j)
            def _(j=j):
                after(j)
        return carry

    for j in range(8):
        if j: got_it(xs.at[j], CHUNK + j)
        expert(j)
        after(j)

    home_from(2, 0, 2)
    home_from(7, 1, 3)
    back_forward()
    home_from(6, 0, 4)
    home_from(3, 1, 5)
    home_forward(2, 2)
    home_forward(7, 3)
    home_from(4, 0, 6)
    home_from(5, 1, 7)
    home_forward(6, 4)
    home_forward(3, 5)
    home_forward(4, 6)
    home_forward(5, 7)

    def combine(s, first):
        r = lax.broadcasted_iota(jnp.int32, (tokens, 8 * cap), 1) + s * 8 * cap
        h0 = jnp.where(code_col[:, 0:1] == r, 1.0, 0.0).astype(jnp.bfloat16)
        h1 = jnp.where(code_col[:, 1:2] == r, 1.0, 0.0).astype(jnp.bfloat16)
        g0, g1 = gates[:, 0:1], gates[:, 1:2]
        for t in range(width // tile):
            cols = pl.ds(t * tile, tile)
            rows = ret[s * 8:(s + 1) * 8, :, cols].reshape(8 * cap, tile)
            v = g0 * jnp.dot(h0, rows, preferred_element_type=jnp.float32) + g1 * jnp.dot(h1, rows, preferred_element_type=jnp.float32)
            if first:
                acc[:, cols] = v
            else:
                acc[:, cols] += v

    for blk, n in locals_:
        pltpu.make_async_copy(back.at[blk, part(0)], ret.at[blk], lsem.at[n]).wait()
    combine(0, True)
    for s in (1, 3, 2):
        for blk in range(8):
            got_it(ret.at[s * 8 + blk], HOME + s * 8 + blk)
        combine(s, False)
    for t in range(width // tile):
        cols = pl.ds(t * tile, tile)
        out[:, cols] = (scale[0] * hid[:, cols].astype(jnp.float32) + scale[1] * acc[:, cols]).astype(out.dtype)
    for src, sid in sent:
        rcopy(src, src, sid, 0, me).wait_send()


def fused(hidden, code, code_col, gates, scale, w1, w3, w2, cap):
    tokens, width = hidden.shape
    ffn = w1.shape[1]
    rows = SIDE * cap
    bf = jnp.bfloat16
    vm = pl.BlockSpec(memory_space=pltpu.VMEM)
    hbm = pl.BlockSpec(memory_space=pl.ANY)
    return pl.pallas_call(
        kernel_body,
        out_shape=[
            jax.ShapeDtypeStruct((tokens, width), bf),
            jax.ShapeDtypeStruct((2, rows, width), bf),
            jax.ShapeDtypeStruct((8, rows, width), bf),
            jax.ShapeDtypeStruct((2, rows, width), bf),
            jax.ShapeDtypeStruct((8, cap, width), bf),
        ],
        in_specs=[vm, vm, vm, vm, pl.BlockSpec(memory_space=pltpu.SMEM), hbm, hbm, hbm],
        out_specs=[vm, hbm, hbm, hbm, hbm],
        scratch_shapes=[
            pltpu.VMEM((width, ffn), bf), pltpu.VMEM((width, ffn), bf), pltpu.VMEM((ffn, width), bf),
            pltpu.VMEM((3, tokens, width), bf),
            pltpu.VMEM((3,) + code.shape, jnp.int32),
            pltpu.VMEM((8 * cap, tokens), bf),
            pltpu.VMEM((8, rows, width), bf),
            pltpu.VMEM((7, rows, width), bf),
            pltpu.VMEM((rows, ffn), bf),
            pltpu.VMEM((32, cap, width), bf),
            pltpu.VMEM((tokens, width), jnp.float32),
            pltpu.SemaphoreType.DMA((NSEND,)),
            pltpu.SemaphoreType.DMA((NMSG,)),
            pltpu.SemaphoreType.DMA((3,)),
            pltpu.SemaphoreType.DMA((8,)),
        ],
        compiler_params=pltpu.CompilerParams(has_side_effects=True, vmem_limit_bytes=67043328),
        name='moe',
    )(hidden, code, code_col, gates, scale, w1, w3, w2)[0]


def route(hidden, router_w, expert_ids, experts, cap):
    tokens, choices = expert_ids.shape
    logits = jnp.dot(hidden.astype(jnp.float32), router_w, precision=lax.Precision.HIGHEST, preferred_element_type=jnp.float32)
    prob = jax.nn.softmax(logits, axis=-1)
    pick = expert_ids[:, :, None] == jnp.arange(experts, dtype=jnp.int32)[None, None, :]
    picked = jnp.sum(jnp.where(pick, prob[:, None, :], 0.0), axis=-1)
    gates = picked / jnp.sum(picked, axis=1, keepdims=True)
    hot = pick.reshape(tokens * choices, experts).astype(jnp.int32)
    earlier = jnp.cumsum(hot, axis=0) - hot
    slot = jnp.sum(earlier * hot, axis=1).reshape(tokens, choices)
    code = expert_ids * cap + slot
    me = lax.axis_index('ep')
    y, x, c = me // (2 * SIDE), (me // 2) % SIDE, me % 2
    ey, ex, ek = expert_ids // (2 * SIDE), (expert_ids // 2) % SIDE, expert_ids % 2
    dy, dx = (ey - y) % SIDE, (ex - x) % SIDE
    dp, dq = jnp.where(c == 0, dx, dy), jnp.where(c == 0, dy, dx)
    code_col = ((dp * SIDE + dq) * 2 + ek) * cap + slot
    return gates, code, code_col


def solution(mesh):
    ep_size = mesh.shape['ep']

    def local_step(hidden, router_w, expert_ids, w_gate, w_up, w_down, post_scale):
        tokens = hidden.shape[0]
        experts = w_gate.shape[0] * ep_size
        cap = tokens // max(1, experts // 8)
        gates, code, code_col = route(hidden, router_w, expert_ids, experts, cap)
        code_rows = jnp.concatenate([code.T, jnp.zeros((6, tokens), jnp.int32)], axis=0)
        return fused(hidden, code_rows, code_col, gates, post_scale, w_gate[0], w_up[0], w_down[0], cap)

    tok_spec = P(('dp', 'ep'))
    return jax.shard_map(local_step, mesh=mesh, in_specs=(tok_spec, P(), tok_spec, P('ep'), P('ep'), P('ep'), P()), out_specs=tok_spec, check_vma=False)
```

```python
import functools
import jax
import jax.numpy as jnp
from jax import lax
from jax.experimental import pallas as pl
from jax.experimental.pallas import tpu as pltpu
from jax.sharding import PartitionSpec as P

MESH = pl.DeviceIdType.MESH
SIDE = 4

CODE = 0
GATHER = 3
CHUNK = 9
LEG = 17
BACK = 19
BLEG = 27
HOPP = 29
HOME = 33
NMSG = 39
SFWD = 39
SBFWD = 41
SNBR = 43
SBACK = 47
NSEND = 54
LHID, LRW, LW1, LW3, LW2, LOUT = 0, 1, 2, 3, 4, 5


def kernel_body(ids, idst, scale, hidh, rwh, w1h, w3h, w2h,
                out, fwd, bleg,
                hid, rw, w1, w3, w2, got, code, codes, gate, pbuf, xs, outq, mid, back, lbuf, rbuf,
                send, recv, lsem):
    tokens, width = hid.shape
    cap = xs.shape[1] // SIDE
    ffn = w1.shape[1]
    experts = rw.shape[1]
    half = tokens // 2
    tile = min(512, width)
    ftile = min(512, ffn)
    f32, bf16 = jnp.float32, jnp.bfloat16
    me = lax.axis_index('ep')
    y, x, c = lax.div(me, 2 * SIDE), lax.rem(lax.div(me, 2), SIDE), lax.rem(me, 2)

    def dev(yy, xx, cc):
        return (lax.rem(yy, SIDE) * SIDE + lax.rem(xx, SIDE)) * 2 + cc

    def qdev(o, core, axis):
        return dev(y + (1 - axis) * o, x + axis * o, core)

    def pdev(o):
        return dev(y + c * o, x + (1 - c) * o, c)

    def rcopy(src, dst, sid, rid, to):
        return pltpu.make_async_remote_copy(src_ref=src, dst_ref=dst, send_sem=send.at[sid], recv_sem=recv.at[rid], device_id={'ep': to}, device_id_type=MESH)

    sent = []

    def put(src, dst, sid, rid, to):
        cp = rcopy(src, dst, sid, rid, to)
        cp.start()
        sent.append((src, sid))

    def drain():
        while sent:
            src, sid = sent.pop(0)
            rcopy(src, src, sid, 0, me).wait_send()

    def got_it(dst, rid):
        rcopy(dst, dst, 0, rid, me).wait_recv()

    def fetch(src, dst, n):
        cp = pltpu.make_async_copy(src, dst, lsem.at[n])
        cp.start()
        return cp

    lo, hi = pl.ds(0, half), pl.ds(half, half)

    barrier = pltpu.get_barrier_semaphore()
    peers = [pdev(1), pdev(2), pdev(3), qdev(0, 1 - c, c)]
    peers += [qdev(o, k, c) for o in (1, 3) for k in range(2)]
    peers += [qdev(o, 1 - c, 1 - c) for o in (1, 3)]
    for to in peers:
        pl.semaphore_signal(barrier, inc=1, device_id={'ep': to}, device_id_type=MESH)
    load_hid = fetch(hidh, hid, LHID)
    load_rw = fetch(rwh, rw, LRW)
    pl.semaphore_wait(barrier, len(peers))

    put(hidh.at[lo], got.at[0, lo], GATHER + 0, GATHER + 0, pdev(1))
    put(hidh.at[hi], got.at[2, hi], GATHER + 2, GATHER + 2, pdev(3))
    put(hidh.at[hi], got.at[0, hi], GATHER + 1, GATHER + 1, pdev(1))
    put(hidh.at[lo], got.at[2, lo], GATHER + 3, GATHER + 3, pdev(3))
    loads = [fetch(w1h, w1, LW1), fetch(w3h, w3, LW3), fetch(w2h, w2, LW2)]

    erow = lax.broadcasted_iota(jnp.int32, (experts, tokens), 0)
    hot0, hot1 = idst[0:1, :] == erow, idst[1:2, :] == erow
    one0, one1 = jnp.where(hot0, 1.0, 0.0), jnp.where(hot1, 1.0, 0.0)
    earlier = lax.broadcasted_iota(jnp.int32, (tokens, tokens), 0) < lax.broadcasted_iota(jnp.int32, (tokens, tokens), 1)
    upper = jnp.where(earlier, 1.0, 0.0).astype(bf16)
    before0 = jnp.dot(one0.astype(bf16), upper, preferred_element_type=f32)
    before1 = jnp.dot(one1.astype(bf16), upper, preferred_element_type=f32) + jnp.sum(one0, axis=1, keepdims=True)
    slot0 = jnp.sum(jnp.where(hot0, before0, 0.0), axis=0, keepdims=True)
    slot1 = jnp.sum(jnp.where(hot1, before1, 0.0), axis=0, keepdims=True)
    code[...] = jnp.zeros(code.shape, jnp.int32)
    code[0:1, :] = idst[0:1, :] * cap + slot0.astype(jnp.int32)
    code[1:2, :] = idst[1:2, :] * cap + slot1.astype(jnp.int32)

    order = (2, 1, 3, 0)

    def code_rows(s):
        return code if s == 0 else codes.at[s - 1]

    def slots(o):
        return lax.broadcasted_iota(jnp.int32, (2 * cap, tokens), 0) + qdev(o, 0, c) * cap

    def pack(s):
        cref = code_rows(s)
        gref = hid if s == 0 else got.at[s - 1]
        c0, c1 = cref[0:1, :], cref[1:2, :]
        for i, o in enumerate(order):
            rows = slots(o)
            pbuf[i * 2 * cap:(i + 1) * 2 * cap, :] = jnp.where((rows == c0) | (rows == c1), 1.0, 0.0).astype(bf16)

        def one(t, carry):
            cols = pl.ds(pl.multiple_of(t * tile, tile), tile)
            r = jnp.dot(pbuf[...], gref[:, cols], preferred_element_type=f32).astype(bf16)
            dst = pl.ds(s * cap, cap)
            for i in range(6):
                outq[i, dst, cols] = r[i * cap:(i + 1) * cap]
            r0, r1 = r[6 * cap:7 * cap], r[7 * cap:8 * cap]
            own0 = c == 0
            xs[0, dst, cols] = jnp.where(own0, r0, r1)
            outq[6, dst, cols] = jnp.where(own0, r1, r0)
            return carry

        lax.fori_loop(0, width // tile, one, 0)

    load_hid.wait()
    pack(0)
    for s, o in ((1, 1), (3, 3), (2, 2)):
        put(code, codes.at[s - 1], CODE + s - 1, CODE + s - 1, pdev(o))
    got_it(got.at[0, lo], GATHER + 0)
    put(got.at[0, lo], got.at[1, lo], GATHER + 4, GATHER + 4, pdev(1))
    got_it(got.at[2, hi], GATHER + 2)
    put(got.at[2, hi], got.at[1, hi], GATHER + 5, GATHER + 5, pdev(3))

    load_rw.wait()
    w = rw[...]
    wa = w.astype(bf16)
    w = w - wa.astype(f32)
    wb = w.astype(bf16)
    wc = (w - wb.astype(f32)).astype(bf16)
    logits = jnp.dot(hid[...], wc, preferred_element_type=f32) + jnp.dot(hid[...], wb, preferred_element_type=f32)
    logits = logits + jnp.dot(hid[...], wa, preferred_element_type=f32)
    ex = jnp.exp(logits - jnp.max(logits, axis=1, keepdims=True))
    prob = ex / jnp.sum(ex, axis=1, keepdims=True)
    ecol = lax.broadcasted_iota(jnp.int32, (tokens, experts), 1)
    p0 = jnp.sum(jnp.where(ids[:, 0:1] == ecol, prob, 0.0), axis=1, keepdims=True)
    p1 = jnp.sum(jnp.where(ids[:, 1:2] == ecol, prob, 0.0), axis=1, keepdims=True)
    gate[0] = jnp.broadcast_to(p0 / (p0 + p1), gate.shape[1:])
    gate[1] = jnp.broadcast_to(p1 / (p0 + p1), gate.shape[1:])

    got_it(codes.at[0], CODE + 0)
    got_it(got.at[0, hi], GATHER + 1)
    pack(1)
    got_it(codes.at[2], CODE + 2)
    got_it(got.at[2, lo], GATHER + 3)
    pack(3)
    got_it(codes.at[1], CODE + 1)
    got_it(got.at[1, lo], GATHER + 4)
    got_it(got.at[1, hi], GATHER + 5)
    pack(2)

    put(outq.at[0], fwd.at[0], LEG + 0, LEG + 0, qdev(1, c, c))
    put(outq.at[1], fwd.at[1], LEG + 1, LEG + 1, qdev(3, c, c))
    put(outq.at[2], xs.at[2 + c], SNBR + 0, CHUNK + 2 + c, qdev(1, 0, c))
    put(outq.at[5], xs.at[2 + c], SNBR + 1, CHUNK + 2 + c, qdev(3, 1, c))
    put(outq.at[6], xs.at[1], CHUNK + 1, CHUNK + 1, qdev(0, 1 - c, c))

    def chunk_forward():
        got_it(fwd.at[0], LEG + 0)
        put(fwd.at[0], xs.at[4 + c], SFWD + 0, CHUNK + 4 + c, qdev(1, 0, c))
        got_it(fwd.at[1], LEG + 1)
        put(fwd.at[1], xs.at[4 + c], SFWD + 1, CHUNK + 4 + c, qdev(3, 1, c))
        put(outq.at[3], xs.at[6 + c], SNBR + 2, CHUNK + 6 + c, qdev(1, 1, c))
        put(outq.at[4], xs.at[6 + c], SNBR + 3, CHUNK + 6 + c, qdev(3, 0, c))

    def back_forward():
        got_it(bleg.at[0], BLEG + 0)
        put(bleg.at[0], back.at[4], SBFWD + 0, BACK + 4, qdev(1, c, c))
        got_it(bleg.at[1], BLEG + 1)
        put(bleg.at[1], back.at[5], SBFWD + 1, BACK + 5, qdev(3, c, c))

    def after(step):
        k = step % 2
        if step == 1:
            put(xs.at[1], back.at[c], SBACK + 0, BACK + c, qdev(0, 1 - c, c))
            chunk_forward()
        elif step in (2, 3):
            put(xs.at[step], back.at[2 + 5 * c], SBACK + step - 1, BACK + 2 + 5 * c, qdev(3 + 2 * c, k, k))
        elif step in (4, 5):
            put(xs.at[step], bleg.at[c], SBACK + step - 1, BLEG + c, qdev(1 + 2 * c, k, k))
        else:
            put(xs.at[step], back.at[6 - 3 * c], SBACK + step - 1, BACK + 6 - 3 * c, qdev(1 + 2 * c, k, k))
            if step == 6:
                back_forward()

    for cp in loads:
        cp.wait()

    def expert(step):
        def up(t, carry):
            cols = pl.ds(pl.multiple_of(t * ftile, ftile), ftile)
            a = jnp.dot(xs[step], w1[:, cols], preferred_element_type=f32)
            b = jnp.dot(xs[step], w3[:, cols], preferred_element_type=f32)
            mid[:, cols] = (jax.nn.silu(a) * b).astype(bf16)
            return carry

        def down(t, carry):
            cols = pl.ds(pl.multiple_of(t * tile, tile), tile)
            r = jnp.dot(mid[...], w2[:, cols], preferred_element_type=f32).astype(bf16)
            if step == 0:
                back[c, :, cols] = r
            else:
                xs[step, :, cols] = r
            return carry

        lax.fori_loop(0, ffn // ftile, up, 0)
        lax.fori_loop(0, width // tile, down, 0)

    for step in range(8):
        if step:
            got_it(xs.at[step], CHUNK + step)
        expert(step)
        if step:
            after(step)

    drain()

    def place(s, k, dst):
        ck = code_rows(s)[k:k + 1, :]
        for o in range(SIDE):
            pbuf[o * 2 * cap:(o + 1) * 2 * cap, :] = jnp.where(slots(o) == ck, 1.0, 0.0).astype(bf16)

        def one(t, carry):
            cols = pl.ds(pl.multiple_of(t * tile, tile), tile)
            rows = back[:, pl.ds(s * cap, cap), cols].reshape(8 * cap, tile)
            dst[:, cols] = lax.dot_general(pbuf[...], rows, (((0,), (0,)), ((), ())), preferred_element_type=f32).astype(bf16)
            return carry

        lax.fori_loop(0, width // tile, one, 0)

    got_it(back.at[1 - c], BACK + 1 - c)
    for blk in (2, 7, 3, 6, 4, 5):
        got_it(back.at[blk], BACK + blk)
    place(2, 0, outq.at[0])
    for i, h in enumerate((lo, hi)):
        put(outq.at[0, h], lbuf.at[0, h], HOPP + i, HOPP + i, pdev(1))
    place(2, 1, outq.at[1])
    for i, h in enumerate((lo, hi)):
        put(outq.at[1, h], lbuf.at[1, h], HOPP + 2 + i, HOPP + 2 + i, pdev(3))
    place(3, 1, outq.at[2])
    put(outq.at[2], rbuf.at[1], HOME + 0, HOME + 0, pdev(1))
    place(1, 0, outq.at[3])
    put(outq.at[3], rbuf.at[2], HOME + 1, HOME + 1, pdev(3))
    place(3, 0, outq.at[4])
    place(1, 1, outq.at[5])
    for i, h in enumerate((lo, hi)):
        got_it(lbuf.at[0, h], HOPP + i)
        outq[4, h, :] = outq[4, h, :] + lbuf[0, h, :]
        put(outq.at[4, h], rbuf.at[0, h], HOME + 2 + i, HOME + 2 + i, pdev(1))
        got_it(lbuf.at[1, h], HOPP + 2 + i)
        outq[5, h, :] = outq[5, h, :] + lbuf[1, h, :]
        put(outq.at[5, h], rbuf.at[3, h], HOME + 4 + i, HOME + 4 + i, pdev(3))
    place(0, 0, got.at[0])
    place(0, 1, got.at[1])
    got_it(rbuf.at[1], HOME + 0)
    got_it(rbuf.at[2], HOME + 1)
    step_rows = min(64, half)
    outs = []
    for i, h in enumerate((lo, hi)):
        got_it(rbuf.at[0, h], HOME + 2 + i)
        got_it(rbuf.at[3, h], HOME + 4 + i)

        def finish(j, carry):
            r = pl.ds(pl.multiple_of(i * half + j * step_rows, step_rows), step_rows)
            g0, g1 = gate[0, r, 0:1], gate[1, r, 0:1]
            for t in range(width // tile):
                cols = pl.ds(t * tile, tile)
                y0 = (got[0, r, cols] + rbuf[0, r, cols] + rbuf[2, r, cols]).astype(f32)
                y1 = (got[1, r, cols] + rbuf[1, r, cols] + rbuf[3, r, cols]).astype(f32)
                mixed = g0 * y0 + g1 * y1
                outq[6, r, cols] = (scale[0] * hid[r, cols].astype(f32) + scale[1] * mixed).astype(bf16)
            return carry

        lax.fori_loop(0, half // step_rows, finish, 0)
        outs.append(fetch(outq.at[6, h], out.at[h], LOUT + i))
    drain()
    for cp in outs:
        cp.wait()


def fused(hidden, rw, ids, idst, scale, w1, w3, w2, cap):
    tokens, width = hidden.shape
    ffn = w1.shape[1]
    rows = SIDE * cap
    bf = jnp.bfloat16
    vm = pl.BlockSpec(memory_space=pltpu.VMEM)
    hbm = pl.BlockSpec(memory_space=pl.ANY)
    return pl.pallas_call(
        kernel_body,
        out_shape=[
            jax.ShapeDtypeStruct((tokens, width), bf),
            jax.ShapeDtypeStruct((2, rows, width), bf),
            jax.ShapeDtypeStruct((2, rows, width), bf),
        ],
        in_specs=[vm, vm, pl.BlockSpec(memory_space=pltpu.SMEM), hbm, hbm, hbm, hbm, hbm],
        out_specs=[hbm, hbm, hbm],
        scratch_shapes=[
            pltpu.VMEM((tokens, width), bf),
            pltpu.VMEM(rw.shape, jnp.float32),
            pltpu.VMEM((width, ffn), bf), pltpu.VMEM((width, ffn), bf), pltpu.VMEM((ffn, width), bf),
            pltpu.VMEM((3, tokens, width), bf),
            pltpu.VMEM(idst.shape, jnp.int32),
            pltpu.VMEM((3,) + idst.shape, jnp.int32),
            pltpu.VMEM((2, tokens, 128), jnp.float32),
            pltpu.VMEM((8 * cap, tokens), bf),
            pltpu.VMEM((8, rows, width), bf),
            pltpu.VMEM((7, rows, width), bf),
            pltpu.VMEM((rows, ffn), bf),
            pltpu.VMEM((8, rows, width), bf),
            pltpu.VMEM((2, tokens, width), bf),
            pltpu.VMEM((4, tokens, width), bf),
            pltpu.SemaphoreType.DMA((NSEND,)),
            pltpu.SemaphoreType.DMA((NMSG,)),
            pltpu.SemaphoreType.DMA((7,)),
        ],
        compiler_params=pltpu.CompilerParams(has_side_effects=True, collective_id=0, vmem_limit_bytes=67043328),
        name='moe',
    )(ids, idst, scale, hidden, rw, w1, w3, w2)[0]


def solution(mesh):
    ep_size = mesh.shape['ep']

    def local_step(hidden, router_w, expert_ids, w_gate, w_up, w_down, post_scale):
        tokens = hidden.shape[0]
        experts = w_gate.shape[0] * ep_size
        cap = tokens // max(1, experts // 8)
        idst = jnp.pad(expert_ids.T, ((0, 6), (0, 0)))
        return fused(hidden, router_w, expert_ids, idst, post_scale, w_gate[0], w_up[0], w_down[0], cap)

    tok_spec = P(('dp', 'ep'))
    return jax.shard_map(local_step, mesh=mesh, in_specs=(tok_spec, P(), tok_spec, P('ep'), P('ep'), P('ep'), P()), out_specs=tok_spec, check_vma=False)
```

```python
import functools
import jax
import jax.numpy as jnp
from jax import lax
from jax.experimental import pallas as pl
from jax.experimental.pallas import tpu as pltpu
from jax.sharding import PartitionSpec as P

MESH = pl.DeviceIdType.MESH
SIDE = 4

CODE = 0
GATHER = 3
CHUNK = 9
LEG = 17
BACK = 21
BLEG = 29
HOPP = 31
HOME = 35
NMSG = 41
SFWD = 41
SBFWD = 43
SNBR = 45
SBACK = 49
NSEND = 56
LHID, LRW, LW1, LW3, LW2, LOUT = 0, 1, 2, 3, 4, 5


def kernel_body(idst, scale, hidh, rwh, w1h, w3h, w2h,
                out, fwd, bleg,
                hid, rw, w1, w3, w2, got, code, codes, gate, pbuf, xs, outq, mid, back, lbuf, rbuf,
                send, recv, lsem):
    tokens, width = hid.shape
    cap = xs.shape[1] // SIDE
    ffn = w1.shape[1]
    experts = rw.shape[0]
    half = tokens // 2
    tile = min(512, width)
    ftile = min(512, ffn)
    f32, bf16 = jnp.float32, jnp.bfloat16
    me = lax.axis_index('ep')
    y, x, c = lax.div(me, 2 * SIDE), lax.rem(lax.div(me, 2), SIDE), lax.rem(me, 2)

    def dev(yy, xx, cc):
        return (lax.rem(yy, SIDE) * SIDE + lax.rem(xx, SIDE)) * 2 + cc

    def qdev(o, core, axis):
        return dev(y + (1 - axis) * o, x + axis * o, core)

    def pdev(o):
        return dev(y + c * o, x + (1 - c) * o, c)

    def rcopy(src, dst, sid, rid, to):
        return pltpu.make_async_remote_copy(src_ref=src, dst_ref=dst, send_sem=send.at[sid], recv_sem=recv.at[rid], device_id={'ep': to}, device_id_type=MESH)

    sent = []

    def put(src, dst, sid, rid, to):
        cp = rcopy(src, dst, sid, rid, to)
        cp.start()
        sent.append((src, sid))

    def drain():
        while sent:
            src, sid = sent.pop(0)
            rcopy(src, src, sid, 0, me).wait_send()

    def got_it(dst, rid):
        rcopy(dst, dst, 0, rid, me).wait_recv()

    def fetch(src, dst, n):
        cp = pltpu.make_async_copy(src, dst, lsem.at[n])
        cp.start()
        return cp

    lo, hi = pl.ds(0, half), pl.ds(half, half)
    first, last = pl.ds(0, 3 * cap), pl.ds(3 * cap, cap)

    def part(s):
        return pl.ds((0, 1, 3, 2)[s] * cap, cap)

    barrier = pltpu.get_barrier_semaphore()
    peers = [pdev(1), pdev(2), pdev(3), qdev(0, 1 - c, c)]
    peers += [qdev(o, k, c) for o in (1, 3) for k in range(2)]
    peers += [qdev(o, 1 - c, 1 - c) for o in (1, 3)]
    for to in peers:
        pl.semaphore_signal(barrier, inc=1, device_id={'ep': to}, device_id_type=MESH)
    load_hid = fetch(hidh, hid, LHID)
    load_rw = fetch(rwh, rw, LRW)
    pl.semaphore_wait(barrier, len(peers))

    put(hidh.at[lo], got.at[0, lo], GATHER + 0, GATHER + 0, pdev(1))
    put(hidh.at[hi], got.at[2, hi], GATHER + 2, GATHER + 2, pdev(3))
    put(hidh.at[hi], got.at[0, hi], GATHER + 1, GATHER + 1, pdev(1))
    put(hidh.at[lo], got.at[2, lo], GATHER + 3, GATHER + 3, pdev(3))
    loads = [fetch(w1h, w1, LW1), fetch(w3h, w3, LW3), fetch(w2h, w2, LW2)]

    erow = lax.broadcasted_iota(jnp.int32, (experts, tokens), 0)
    hot0, hot1 = idst[0:1, :] == erow, idst[1:2, :] == erow
    one0, one1 = jnp.where(hot0, 1.0, 0.0), jnp.where(hot1, 1.0, 0.0)
    earlier = lax.broadcasted_iota(jnp.int32, (tokens, tokens), 0) < lax.broadcasted_iota(jnp.int32, (tokens, tokens), 1)
    upper = jnp.where(earlier, 1.0, 0.0).astype(bf16)
    before0 = jnp.dot(one0.astype(bf16), upper, preferred_element_type=f32)
    before1 = jnp.dot(one1.astype(bf16), upper, preferred_element_type=f32) + jnp.sum(one0, axis=1, keepdims=True)
    slot0 = jnp.sum(jnp.where(hot0, before0, 0.0), axis=0, keepdims=True)
    slot1 = jnp.sum(jnp.where(hot1, before1, 0.0), axis=0, keepdims=True)
    code[...] = jnp.zeros(code.shape, jnp.int32)
    code[0:1, :] = idst[0:1, :] * cap + slot0.astype(jnp.int32)
    code[1:2, :] = idst[1:2, :] * cap + slot1.astype(jnp.int32)

    order = (2, 1, 3, 0)

    def code_rows(s):
        return code if s == 0 else codes.at[s - 1]

    def slots(o, n=tokens):
        return lax.broadcasted_iota(jnp.int32, (2 * cap, n), 0) + qdev(o, 0, c) * cap

    def pack(s):
        cref = code_rows(s)
        gref = hid if s == 0 else got.at[s - 1]
        c0, c1 = cref[0:1, :], cref[1:2, :]
        for i, o in enumerate(order):
            rows = slots(o)
            pbuf[i * 2 * cap:(i + 1) * 2 * cap, :] = jnp.where((rows == c0) | (rows == c1), 1.0, 0.0).astype(bf16)

        def one(t, carry):
            cols = pl.ds(pl.multiple_of(t * tile, tile), tile)
            r = jnp.dot(pbuf[...], gref[:, cols], preferred_element_type=f32).astype(bf16)
            dst = part(s)
            for i in range(6):
                outq[i, dst, cols] = r[i * cap:(i + 1) * cap]
            r0, r1 = r[6 * cap:7 * cap], r[7 * cap:8 * cap]
            own0 = c == 0
            xs[0, dst, cols] = jnp.where(own0, r0, r1)
            outq[6, dst, cols] = jnp.where(own0, r1, r0)
            return carry

        lax.fori_loop(0, width // tile, one, 0)

    load_hid.wait()
    pack(0)
    for s, o in ((1, 1), (3, 3), (2, 2)):
        put(code, codes.at[s - 1], CODE + s - 1, CODE + s - 1, pdev(o))
    got_it(got.at[0, lo], GATHER + 0)
    put(got.at[0, lo], got.at[1, lo], GATHER + 4, GATHER + 4, pdev(1))
    got_it(got.at[2, hi], GATHER + 2)
    put(got.at[2, hi], got.at[1, hi], GATHER + 5, GATHER + 5, pdev(3))

    load_rw.wait()
    w = rw[...]
    wa = w.astype(bf16)
    w = w - wa.astype(f32)
    wb = w.astype(bf16)
    wc = (w - wb.astype(f32)).astype(bf16)
    terms = lax.dot_general(jnp.concatenate([wc, wb, wa], axis=0), hid[...], (((1,), (1,)), ((), ())), preferred_element_type=f32)
    logits = (terms[0:experts] + terms[experts:2 * experts]) + terms[2 * experts:]
    ex = jnp.exp(logits - jnp.max(logits, axis=0, keepdims=True))
    prob = ex / jnp.sum(ex, axis=0, keepdims=True)
    p0 = jnp.sum(jnp.where(hot0, prob, 0.0), axis=0, keepdims=True)
    p1 = jnp.sum(jnp.where(hot1, prob, 0.0), axis=0, keepdims=True)
    gate[0] = jnp.broadcast_to(p0 / (p0 + p1), (128, tokens)).T
    gate[1] = jnp.broadcast_to(p1 / (p0 + p1), (128, tokens)).T

    got_it(codes.at[0], CODE + 0)
    got_it(got.at[0, hi], GATHER + 1)
    pack(1)
    got_it(codes.at[2], CODE + 2)
    got_it(got.at[2, lo], GATHER + 3)
    pack(3)
    put(outq.at[0, first], fwd.at[0, first], LEG + 0, LEG + 0, qdev(1, c, c))
    put(outq.at[1, first], fwd.at[1, first], LEG + 1, LEG + 1, qdev(3, c, c))
    got_it(codes.at[1], CODE + 1)
    got_it(got.at[1, lo], GATHER + 4)
    got_it(got.at[1, hi], GATHER + 5)
    pack(2)

    put(outq.at[0, last], fwd.at[0, last], LEG + 2, LEG + 2, qdev(1, c, c))
    put(outq.at[1, last], fwd.at[1, last], LEG + 3, LEG + 3, qdev(3, c, c))
    put(outq.at[2], xs.at[2 + c], SNBR + 0, CHUNK + 2 + c, qdev(1, 0, c))
    put(outq.at[5], xs.at[2 + c], SNBR + 1, CHUNK + 2 + c, qdev(3, 1, c))
    put(outq.at[6], xs.at[1], CHUNK + 1, CHUNK + 1, qdev(0, 1 - c, c))

    def chunk_forward():
        got_it(fwd.at[0, first], LEG + 0)
        got_it(fwd.at[0, last], LEG + 2)
        put(fwd.at[0], xs.at[4 + c], SFWD + 0, CHUNK + 4 + c, qdev(1, 0, c))
        got_it(fwd.at[1, first], LEG + 1)
        got_it(fwd.at[1, last], LEG + 3)
        put(fwd.at[1], xs.at[4 + c], SFWD + 1, CHUNK + 4 + c, qdev(3, 1, c))
        put(outq.at[3], xs.at[6 + c], SNBR + 2, CHUNK + 6 + c, qdev(1, 1, c))
        put(outq.at[4], xs.at[6 + c], SNBR + 3, CHUNK + 6 + c, qdev(3, 0, c))

    def back_forward():
        got_it(bleg.at[0], BLEG + 0)
        put(bleg.at[0], back.at[4], SBFWD + 0, BACK + 4, qdev(1, c, c))
        got_it(bleg.at[1], BLEG + 1)
        put(bleg.at[1], back.at[5], SBFWD + 1, BACK + 5, qdev(3, c, c))

    def after(step):
        k = step % 2
        if step == 1:
            put(xs.at[1], back.at[c], SBACK + 0, BACK + c, qdev(0, 1 - c, c))
            chunk_forward()
        elif step in (2, 3):
            put(xs.at[step], back.at[2 + 5 * c], SBACK + step - 1, BACK + 2 + 5 * c, qdev(3 + 2 * c, k, k))
        elif step in (4, 5):
            put(xs.at[step], bleg.at[c], SBACK + step - 1, BLEG + c, qdev(1 + 2 * c, k, k))
        else:
            put(xs.at[step], back.at[6 - 3 * c], SBACK + step - 1, BACK + 6 - 3 * c, qdev(1 + 2 * c, k, k))
            if step == 6:
                back_forward()

    for cp in loads:
        cp.wait()

    def expert(step):
        def up(t, carry):
            cols = pl.ds(pl.multiple_of(t * ftile, ftile), ftile)
            a = jnp.dot(xs[step], w1[:, cols], preferred_element_type=f32)
            b = jnp.dot(xs[step], w3[:, cols], preferred_element_type=f32)
            mid[:, cols] = (jax.nn.silu(a) * b).astype(bf16)
            return carry

        def down(t, carry):
            cols = pl.ds(pl.multiple_of(t * tile, tile), tile)
            r = jnp.dot(mid[...], w2[:, cols], preferred_element_type=f32).astype(bf16)
            if step == 0:
                back[c, :, cols] = r
            else:
                xs[step, :, cols] = r
            return carry

        lax.fori_loop(0, ffn // ftile, up, 0)
        lax.fori_loop(0, width // tile, down, 0)

    for step in (0, 1, 2, 3, 5, 4, 6, 7):
        if step:
            got_it(xs.at[step], CHUNK + step)
        expert(step)
        if step:
            after(step)

    drain()

    def place(s, k, dst, i=0, n=tokens):
        ck = code_rows(s)[k:k + 1, i * n:(i + 1) * n]
        for o in range(SIDE):
            pbuf[o * 2 * cap:(o + 1) * 2 * cap, 0:n] = jnp.where(slots(o, n) == ck, 1.0, 0.0).astype(bf16)

        def one(t, carry):
            cols = pl.ds(pl.multiple_of(t * tile, tile), tile)
            rows = back[:, part(s), cols].reshape(8 * cap, tile)
            dst[i * n:(i + 1) * n, cols] = lax.dot_general(pbuf[:, 0:n], rows, (((0,), (0,)), ((), ())), preferred_element_type=f32).astype(bf16)
            return carry

        lax.fori_loop(0, width // tile, one, 0)

    got_it(back.at[1 - c], BACK + 1 - c)
    for blk in (2, 7, 3, 6, 4, 5):
        got_it(back.at[blk], BACK + blk)
    for i, h in enumerate((lo, hi)):
        place(2, 0, outq.at[0], i, half)
        put(outq.at[0, h], lbuf.at[0, h], HOPP + i, HOPP + i, pdev(1))
        place(2, 1, outq.at[1], i, half)
        put(outq.at[1, h], lbuf.at[1, h], HOPP + 2 + i, HOPP + 2 + i, pdev(3))
    place(3, 1, outq.at[2])
    put(outq.at[2], rbuf.at[1], HOME + 0, HOME + 0, pdev(1))
    place(1, 0, outq.at[3])
    put(outq.at[3], rbuf.at[2], HOME + 1, HOME + 1, pdev(3))
    place(3, 0, outq.at[4])
    place(1, 1, outq.at[5])
    for i, h in enumerate((lo, hi)):
        got_it(lbuf.at[0, h], HOPP + i)
        outq[4, h, :] = outq[4, h, :] + lbuf[0, h, :]
        put(outq.at[4, h], rbuf.at[0, h], HOME + 2 + i, HOME + 2 + i, pdev(1))
        got_it(lbuf.at[1, h], HOPP + 2 + i)
        outq[5, h, :] = outq[5, h, :] + lbuf[1, h, :]
        put(outq.at[5, h], rbuf.at[3, h], HOME + 4 + i, HOME + 4 + i, pdev(3))
    place(0, 0, got.at[0])
    place(0, 1, got.at[1])
    got_it(rbuf.at[1], HOME + 0)
    got_it(rbuf.at[2], HOME + 1)
    step_rows = min(64, half)
    outs = []
    for i, h in enumerate((lo, hi)):
        got_it(rbuf.at[0, h], HOME + 2 + i)
        got_it(rbuf.at[3, h], HOME + 4 + i)

        def finish(j, carry):
            r = pl.ds(pl.multiple_of(i * half + j * step_rows, step_rows), step_rows)
            g0, g1 = gate[0, r, 0:1], gate[1, r, 0:1]
            for t in range(width // tile):
                cols = pl.ds(t * tile, tile)
                y0 = (got[0, r, cols] + rbuf[0, r, cols] + rbuf[2, r, cols]).astype(f32)
                y1 = (got[1, r, cols] + rbuf[1, r, cols] + rbuf[3, r, cols]).astype(f32)
                mixed = g0 * y0 + g1 * y1
                outq[6, r, cols] = (scale[0] * hid[r, cols].astype(f32) + scale[1] * mixed).astype(bf16)
            return carry

        lax.fori_loop(0, half // step_rows, finish, 0)
        outs.append(fetch(outq.at[6, h], out.at[h], LOUT + i))
    drain()
    for cp in outs:
        cp.wait()


def fused(hidden, rw, idst, scale, w1, w3, w2, cap):
    tokens, width = hidden.shape
    ffn = w1.shape[1]
    rows = SIDE * cap
    bf = jnp.bfloat16
    vm = pl.BlockSpec(memory_space=pltpu.VMEM)
    hbm = pl.BlockSpec(memory_space=pl.ANY)
    return pl.pallas_call(
        kernel_body,
        out_shape=[
            jax.ShapeDtypeStruct((tokens, width), bf),
            jax.ShapeDtypeStruct((2, rows, width), bf),
            jax.ShapeDtypeStruct((2, rows, width), bf),
        ],
        in_specs=[vm, pl.BlockSpec(memory_space=pltpu.SMEM), hbm, hbm, hbm, hbm, hbm],
        out_specs=[hbm, hbm, hbm],
        scratch_shapes=[
            pltpu.VMEM((tokens, width), bf),
            pltpu.VMEM(rw.shape, jnp.float32),
            pltpu.VMEM((width, ffn), bf), pltpu.VMEM((width, ffn), bf), pltpu.VMEM((ffn, width), bf),
            pltpu.VMEM((3, tokens, width), bf),
            pltpu.VMEM((8, tokens), jnp.int32),
            pltpu.VMEM((3, 8, tokens), jnp.int32),
            pltpu.VMEM((2, tokens, 128), jnp.float32),
            pltpu.VMEM((8 * cap, tokens), bf),
            pltpu.VMEM((8, rows, width), bf),
            pltpu.VMEM((7, rows, width), bf),
            pltpu.VMEM((rows, ffn), bf),
            pltpu.VMEM((8, rows, width), bf),
            pltpu.VMEM((2, tokens, width), bf),
            pltpu.VMEM((4, tokens, width), bf),
            pltpu.SemaphoreType.DMA((NSEND,)),
            pltpu.SemaphoreType.DMA((NMSG,)),
            pltpu.SemaphoreType.DMA((7,)),
        ],
        compiler_params=pltpu.CompilerParams(has_side_effects=True, collective_id=0, vmem_limit_bytes=67043328),
        name='moe',
    )(idst, scale, hidden, rw, w1, w3, w2)[0]


def solution(mesh):
    ep_size = mesh.shape['ep']

    def local_step(hidden, router_w, expert_ids, w_gate, w_up, w_down, post_scale):
        tokens = hidden.shape[0]
        experts = w_gate.shape[0] * ep_size
        cap = tokens // max(1, experts // 8)
        return fused(hidden, router_w.T, expert_ids.T, post_scale, w_gate[0], w_up[0], w_down[0], cap)

    tok_spec = P(('dp', 'ep'))
    return jax.shard_map(local_step, mesh=mesh, in_specs=(tok_spec, P(), tok_spec, P('ep'), P('ep'), P('ep'), P()), out_specs=tok_spec, check_vma=False)
```

```python
import functools
import jax
import jax.numpy as jnp
from jax import lax
from jax.experimental import pallas as pl
from jax.experimental.pallas import tpu as pltpu
from jax.sharding import PartitionSpec as P

MESH = pl.DeviceIdType.MESH
SIDE = 4

CODE = 0
GATHER = 3
CHUNK = 9
LEG = 17
BACK = 21
BLEG = 37
HOPP = 41
HOME = 45
NMSG = 53
SFWD = 53
SBFWD = 55
SNBR = 59
SBACK = 63
NSEND = 77
LHID, LRW, LW1, LW3, LW2, LOUT = 0, 1, 2, 3, 4, 5


def kernel_body(idst, scale, hidh, rwh, w1h, w3h, w2h,
                out, fwd, bleg,
                hid, rw, w1, w3, w2, got, code, codes, gate, pbuf, xs, outq, mid, back, lbuf, rbuf,
                send, recv, lsem):
    tokens, width = hid.shape
    cap = xs.shape[1] // SIDE
    ffn = w1.shape[1]
    experts = rw.shape[0]
    half = tokens // 2
    tile = min(512, width // 2)
    wide = width // 2
    sides = (pl.ds(0, wide), pl.ds(wide, wide))
    ftile = min(512, ffn)
    f32, bf16 = jnp.float32, jnp.bfloat16
    me = lax.axis_index('ep')
    y, x, c = lax.div(me, 2 * SIDE), lax.rem(lax.div(me, 2), SIDE), lax.rem(me, 2)

    def dev(yy, xx, cc):
        return (lax.rem(yy, SIDE) * SIDE + lax.rem(xx, SIDE)) * 2 + cc

    def qdev(o, core, axis):
        return dev(y + (1 - axis) * o, x + axis * o, core)

    def pdev(o):
        return dev(y + c * o, x + (1 - c) * o, c)

    def rcopy(src, dst, sid, rid, to):
        return pltpu.make_async_remote_copy(src_ref=src, dst_ref=dst, send_sem=send.at[sid], recv_sem=recv.at[rid], device_id={'ep': to}, device_id_type=MESH)

    sent = []

    def put(src, dst, sid, rid, to):
        cp = rcopy(src, dst, sid, rid, to)
        cp.start()
        sent.append((src, sid))

    def drain(n=None):
        for _ in range(len(sent) if n is None else n):
            src, sid = sent.pop(0)
            rcopy(src, src, sid, 0, me).wait_send()

    def got_it(dst, rid):
        rcopy(dst, dst, 0, rid, me).wait_recv()

    def fetch(src, dst, n):
        cp = pltpu.make_async_copy(src, dst, lsem.at[n])
        cp.start()
        return cp

    lo, hi = pl.ds(0, half), pl.ds(half, half)
    first, last = pl.ds(0, 3 * cap), pl.ds(3 * cap, cap)

    def part(s):
        return pl.ds((0, 1, 3, 2)[s] * cap, cap)

    barrier = pltpu.get_barrier_semaphore()
    peers = [pdev(1), pdev(2), pdev(3), qdev(0, 1 - c, c)]
    peers += [qdev(o, k, c) for o in (1, 3) for k in range(2)]
    peers += [qdev(o, 1 - c, 1 - c) for o in (1, 3)]
    for to in peers:
        pl.semaphore_signal(barrier, inc=1, device_id={'ep': to}, device_id_type=MESH)
    load_hid = fetch(hidh, hid, LHID)
    load_rw = fetch(rwh, rw, LRW)
    pl.semaphore_wait(barrier, len(peers))

    put(hidh.at[lo], got.at[0, lo], GATHER + 0, GATHER + 0, pdev(1))
    put(hidh.at[hi], got.at[2, hi], GATHER + 2, GATHER + 2, pdev(3))
    put(hidh.at[hi], got.at[0, hi], GATHER + 1, GATHER + 1, pdev(1))
    put(hidh.at[lo], got.at[2, lo], GATHER + 3, GATHER + 3, pdev(3))
    loads = [fetch(w1h, w1, LW1), fetch(w3h, w3, LW3), fetch(w2h, w2, LW2)]

    erow = lax.broadcasted_iota(jnp.int32, (experts, tokens), 0)
    hot0, hot1 = idst[0:1, :] == erow, idst[1:2, :] == erow
    one0, one1 = jnp.where(hot0, 1.0, 0.0), jnp.where(hot1, 1.0, 0.0)
    earlier = lax.broadcasted_iota(jnp.int32, (tokens, tokens), 0) < lax.broadcasted_iota(jnp.int32, (tokens, tokens), 1)
    upper = jnp.where(earlier, 1.0, 0.0).astype(bf16)
    before0 = jnp.dot(one0.astype(bf16), upper, preferred_element_type=f32)
    before1 = jnp.dot(one1.astype(bf16), upper, preferred_element_type=f32) + jnp.sum(one0, axis=1, keepdims=True)
    slot0 = jnp.sum(jnp.where(hot0, before0, 0.0), axis=0, keepdims=True)
    slot1 = jnp.sum(jnp.where(hot1, before1, 0.0), axis=0, keepdims=True)
    code[...] = jnp.zeros(code.shape, jnp.int32)
    code[0:1, :] = idst[0:1, :] * cap + slot0.astype(jnp.int32)
    code[1:2, :] = idst[1:2, :] * cap + slot1.astype(jnp.int32)

    order = (2, 1, 3, 0)

    def code_rows(s):
        return code if s == 0 else codes.at[s - 1]

    def slots(o, n=tokens):
        return lax.broadcasted_iota(jnp.int32, (2 * cap, n), 0) + qdev(o, 0, c) * cap

    def pack(s):
        cref = code_rows(s)
        gref = hid if s == 0 else got.at[s - 1]
        c0, c1 = cref[0:1, :], cref[1:2, :]
        for i, o in enumerate(order):
            rows = slots(o)
            pbuf[i * 2 * cap:(i + 1) * 2 * cap, :] = jnp.where((rows == c0) | (rows == c1), 1.0, 0.0).astype(bf16)

        def one(t, carry):
            cols = pl.ds(pl.multiple_of(t * tile, tile), tile)
            r = jnp.dot(pbuf[...], gref[:, cols], preferred_element_type=f32).astype(bf16)
            dst = part(s)
            for i in range(6):
                outq[i, dst, cols] = r[i * cap:(i + 1) * cap]
            r0, r1 = r[6 * cap:7 * cap], r[7 * cap:8 * cap]
            own0 = c == 0
            xs[0, dst, cols] = jnp.where(own0, r0, r1)
            outq[6, dst, cols] = jnp.where(own0, r1, r0)
            return carry

        lax.fori_loop(0, width // tile, one, 0)

    load_hid.wait()
    pack(0)
    for s, o in ((1, 1), (3, 3), (2, 2)):
        put(code, codes.at[s - 1], CODE + s - 1, CODE + s - 1, pdev(o))
    got_it(got.at[0, lo], GATHER + 0)
    put(got.at[0, lo], got.at[1, lo], GATHER + 4, GATHER + 4, pdev(1))
    got_it(got.at[2, hi], GATHER + 2)
    put(got.at[2, hi], got.at[1, hi], GATHER + 5, GATHER + 5, pdev(3))

    load_rw.wait()
    w = rw[...]
    wa = w.astype(bf16)
    w = w - wa.astype(f32)
    wb = w.astype(bf16)
    wc = (w - wb.astype(f32)).astype(bf16)
    terms = lax.dot_general(jnp.concatenate([wc, wb, wa], axis=0), hid[...], (((1,), (1,)), ((), ())), preferred_element_type=f32)
    logits = (terms[0:experts] + terms[experts:2 * experts]) + terms[2 * experts:]
    ex = jnp.exp(logits - jnp.max(logits, axis=0, keepdims=True))
    prob = ex / jnp.sum(ex, axis=0, keepdims=True)
    p0 = jnp.sum(jnp.where(hot0, prob, 0.0), axis=0, keepdims=True)
    p1 = jnp.sum(jnp.where(hot1, prob, 0.0), axis=0, keepdims=True)
    gate[0] = jnp.broadcast_to(p0 / (p0 + p1), (128, tokens)).T
    gate[1] = jnp.broadcast_to(p1 / (p0 + p1), (128, tokens)).T

    got_it(codes.at[0], CODE + 0)
    got_it(got.at[0, hi], GATHER + 1)
    pack(1)
    got_it(codes.at[2], CODE + 2)
    got_it(got.at[2, lo], GATHER + 3)
    pack(3)
    put(outq.at[0, first], fwd.at[0, first], LEG + 0, LEG + 0, qdev(1, c, c))
    put(outq.at[1, first], fwd.at[1, first], LEG + 1, LEG + 1, qdev(3, c, c))
    got_it(codes.at[1], CODE + 1)
    got_it(got.at[1, lo], GATHER + 4)
    got_it(got.at[1, hi], GATHER + 5)
    pack(2)

    put(outq.at[0, last], fwd.at[0, last], LEG + 2, LEG + 2, qdev(1, c, c))
    put(outq.at[1, last], fwd.at[1, last], LEG + 3, LEG + 3, qdev(3, c, c))
    put(outq.at[2], xs.at[2 + c], SNBR + 0, CHUNK + 2 + c, qdev(1, 0, c))
    put(outq.at[5], xs.at[2 + c], SNBR + 1, CHUNK + 2 + c, qdev(3, 1, c))
    put(outq.at[6], xs.at[1], CHUNK + 1, CHUNK + 1, qdev(0, 1 - c, c))

    def chunk_forward():
        got_it(fwd.at[0, first], LEG + 0)
        got_it(fwd.at[0, last], LEG + 2)
        put(fwd.at[0], xs.at[4 + c], SFWD + 0, CHUNK + 4 + c, qdev(1, 0, c))
        got_it(fwd.at[1, first], LEG + 1)
        got_it(fwd.at[1, last], LEG + 3)
        put(fwd.at[1], xs.at[4 + c], SFWD + 1, CHUNK + 4 + c, qdev(3, 1, c))
        put(outq.at[3], xs.at[6 + c], SNBR + 2, CHUNK + 6 + c, qdev(1, 1, c))
        put(outq.at[4], xs.at[6 + c], SNBR + 3, CHUNK + 6 + c, qdev(3, 0, c))

    def back_forward(f):
        for i, o in enumerate((1, 3)):
            got_it(bleg.at[i, :, sides[f]], BLEG + 2 * f + i)
            put(bleg.at[i, :, sides[f]], back.at[4 + i, :, sides[f]], SBFWD + 2 * f + i, BACK + 8 * f + 4 + i, qdev(o, c, c))

    def after(step, f):
        k, sid = step % 2, SBACK + 2 * (step - 1)
        if step == 1:
            put(xs.at[1], back.at[c], sid, BACK + c, qdev(0, 1 - c, c))
        elif step in (2, 3):
            put(xs.at[step], back.at[2 + 5 * c], sid, BACK + 2 + 5 * c, qdev(3 + 2 * c, k, k))
        elif step in (4, 5):
            put(xs.at[step, :, sides[f]], bleg.at[c, :, sides[f]], sid + f, BLEG + 2 * f + c, qdev(1 + 2 * c, k, k))
        else:
            put(xs.at[step, :, sides[f]], back.at[6 - 3 * c, :, sides[f]], sid + f, BACK + 8 * f + 6 - 3 * c, qdev(1 + 2 * c, k, k))

    for cp in loads:
        cp.wait()

    def expert(step):
        def up(t, carry):
            cols = pl.ds(pl.multiple_of(t * ftile, ftile), ftile)
            a = jnp.dot(xs[step], w1[:, cols], preferred_element_type=f32)
            b = jnp.dot(xs[step], w3[:, cols], preferred_element_type=f32)
            mid[:, cols] = (jax.nn.silu(a) * b).astype(bf16)
            return carry

        def down(t, carry):
            cols = pl.ds(pl.multiple_of(t * tile, tile), tile)
            r = jnp.dot(mid[...], w2[:, cols], preferred_element_type=f32).astype(bf16)
            if step == 0:
                back[c, :, cols] = r
            else:
                xs[step, :, cols] = r
            return carry

        lax.fori_loop(0, ffn // ftile, up, 0)
        if step == 7:
            back_forward(1)
        tiles = width // tile
        if step < 4:
            lax.fori_loop(0, tiles, down, 0)
            if step:
                after(step, 0)
        else:
            lax.fori_loop(0, tiles // 2, down, 0)
            after(step, 0)
            lax.fori_loop(tiles // 2, tiles, down, 0)
            after(step, 1)

    for step in range(8):
        if step:
            got_it(xs.at[step], CHUNK + step)
        expert(step)
        if step == 1:
            chunk_forward()
            chunks_sent = len(sent)
        elif step == 6:
            back_forward(0)

    drain(chunks_sent)

    def place(s, k, dst, f):
        ck = code_rows(s)[k:k + 1, :]
        for o in range(SIDE):
            pbuf[o * 2 * cap:(o + 1) * 2 * cap, :] = jnp.where(slots(o) == ck, 1.0, 0.0).astype(bf16)

        def one(t, carry):
            cols = pl.ds(pl.multiple_of(f * wide + t * tile, tile), tile)
            rows = back[:, part(s), cols].reshape(8 * cap, tile)
            dst[:, cols] = lax.dot_general(pbuf[...], rows, (((0,), (0,)), ((), ())), preferred_element_type=f32).astype(bf16)
            return carry

        lax.fori_loop(0, wide // tile, one, 0)

    def unmerged(f):
        h = sides[f]
        for i, (k, o) in enumerate(((0, 1), (1, 3))):
            place(2, k, outq.at[i], f)
            put(outq.at[i, :, h], lbuf.at[i, :, h], HOPP + 2 * f + i, HOPP + 2 * f + i, pdev(o))
        for i, (s, k, o) in enumerate(((3, 1, 1), (1, 0, 3))):
            place(s, k, outq.at[2 + i], f)
            put(outq.at[2 + i, :, h], rbuf.at[1 + i, :, h], HOME + 2 * f + i, HOME + 2 * f + i, pdev(o))

    def mergeable(f):
        place(3, 0, outq.at[4], f)
        place(1, 1, outq.at[5], f)

    def merged(f):
        h = sides[f]
        for i, o in enumerate((1, 3)):
            got_it(lbuf.at[i, :, h], HOPP + 2 * f + i)
            outq[4 + i, :, h] = outq[4 + i, :, h] + lbuf[i, :, h]
            put(outq.at[4 + i, :, h], rbuf.at[3 * i, :, h], HOME + 4 + 2 * f + i, HOME + 4 + 2 * f + i, pdev(o))

    got_it(back.at[1 - c], BACK + 1 - c)
    for blk in (2, 7):
        got_it(back.at[blk], BACK + blk)
    for f in range(2):
        for blk in (3, 6, 4, 5):
            got_it(back.at[blk, :, sides[f]], BACK + 8 * f + blk)
        unmerged(f)
        if f == 0:
            mergeable(0)
    merged(0)
    mergeable(1)
    merged(1)
    for k in range(2):
        for f in range(2):
            place(0, k, got.at[k], f)
    step_rows = min(64, tokens)
    outs = []
    for f in range(2):
        h = sides[f]
        for i in range(2):
            got_it(rbuf.at[1 + i, :, h], HOME + 2 * f + i)
        for i in range(2):
            got_it(rbuf.at[3 * i, :, h], HOME + 4 + 2 * f + i)

        def finish(j, carry):
            r = pl.ds(pl.multiple_of(j * step_rows, step_rows), step_rows)
            g0, g1 = gate[0, r, 0:1], gate[1, r, 0:1]
            for t in range(wide // tile):
                cols = pl.ds(f * wide + t * tile, tile)
                y0 = (got[0, r, cols] + rbuf[0, r, cols] + rbuf[2, r, cols]).astype(f32)
                y1 = (got[1, r, cols] + rbuf[1, r, cols] + rbuf[3, r, cols]).astype(f32)
                mixed = g0 * y0 + g1 * y1
                outq[6, r, cols] = (scale[0] * hid[r, cols].astype(f32) + scale[1] * mixed).astype(bf16)
            return carry

        lax.fori_loop(0, tokens // step_rows, finish, 0)
        outs.append(fetch(outq.at[6, :, h], out.at[:, h], LOUT + f))
    drain()
    for cp in outs:
        cp.wait()


def fused(hidden, rw, idst, scale, w1, w3, w2, cap):
    tokens, width = hidden.shape
    ffn = w1.shape[1]
    rows = SIDE * cap
    bf = jnp.bfloat16
    vm = pl.BlockSpec(memory_space=pltpu.VMEM)
    hbm = pl.BlockSpec(memory_space=pl.ANY)
    return pl.pallas_call(
        kernel_body,
        out_shape=[
            jax.ShapeDtypeStruct((tokens, width), bf),
            jax.ShapeDtypeStruct((2, rows, width), bf),
            jax.ShapeDtypeStruct((2, rows, width), bf),
        ],
        in_specs=[vm, pl.BlockSpec(memory_space=pltpu.SMEM), hbm, hbm, hbm, hbm, hbm],
        out_specs=[hbm, hbm, hbm],
        scratch_shapes=[
            pltpu.VMEM((tokens, width), bf),
            pltpu.VMEM(rw.shape, jnp.float32),
            pltpu.VMEM((width, ffn), bf), pltpu.VMEM((width, ffn), bf), pltpu.VMEM((ffn, width), bf),
            pltpu.VMEM((3, tokens, width), bf),
            pltpu.VMEM((8, tokens), jnp.int32),
            pltpu.VMEM((3, 8, tokens), jnp.int32),
            pltpu.VMEM((2, tokens, 128), jnp.float32),
            pltpu.VMEM((8 * cap, tokens), bf),
            pltpu.VMEM((8, rows, width), bf),
            pltpu.VMEM((7, rows, width), bf),
            pltpu.VMEM((rows, ffn), bf),
            pltpu.VMEM((8, rows, width), bf),
            pltpu.VMEM((2, tokens, width), bf),
            pltpu.VMEM((4, tokens, width), bf),
            pltpu.SemaphoreType.DMA((NSEND,)),
            pltpu.SemaphoreType.DMA((NMSG,)),
            pltpu.SemaphoreType.DMA((7,)),
        ],
        compiler_params=pltpu.CompilerParams(has_side_effects=True, collective_id=0, vmem_limit_bytes=67043328),
        name='moe',
    )(idst, scale, hidden, rw, w1, w3, w2)[0]


def solution(mesh):
    ep_size = mesh.shape['ep']

    def local_step(hidden, router_w, expert_ids, w_gate, w_up, w_down, post_scale):
        tokens = hidden.shape[0]
        experts = w_gate.shape[0] * ep_size
        cap = tokens // max(1, experts // 8)
        return fused(hidden, router_w.T, expert_ids.T, post_scale, w_gate[0], w_up[0], w_down[0], cap)

    tok_spec = P(('dp', 'ep'))
    return jax.shard_map(local_step, mesh=mesh, in_specs=(tok_spec, P(), tok_spec, P('ep'), P('ep'), P('ep'), P()), out_specs=tok_spec, check_vma=False)
```

```python
import functools
import jax
import jax.numpy as jnp
from jax import lax
from jax.experimental import pallas as pl
from jax.experimental.pallas import tpu as pltpu
from jax.sharding import PartitionSpec as P

MESH = pl.DeviceIdType.MESH
SIDE = 4

CODE = 0
GATHER = 3
CHUNK = 9
LEG = 17
BACK = 21
BLEG = 37
HOPP = 41
HOME = 45
NMSG = 53
SFWD = 53
SBFWD = 55
SNBR = 59
SBACK = 63
NSEND = 77
LHID, LRW, LW1, LW3, LW2, LOUT, LIDS = 0, 1, 2, 3, 4, 5, 7


def kernel_body(idsh, scale, hidh, rwh, w1h, w3h, w2h,
                out, fwd, bleg,
                idst, hid, rw, w1, w3, w2, got, code, codes, gate, pbuf, xs, outq, mid, back, lbuf, rbuf,
                send, recv, lsem):
    tokens, width = hid.shape
    cap = xs.shape[1] // SIDE
    ffn = w1.shape[1]
    experts = rw.shape[0]
    half = tokens // 2
    tile = min(512, width // 2)
    wide = width // 2
    sides = (pl.ds(0, wide), pl.ds(wide, wide))
    ftile = min(512, ffn)
    f32, bf16 = jnp.float32, jnp.bfloat16
    me = lax.axis_index('ep')
    y, x, c = lax.div(me, 2 * SIDE), lax.rem(lax.div(me, 2), SIDE), lax.rem(me, 2)

    def dev(yy, xx, cc):
        return (lax.rem(yy, SIDE) * SIDE + lax.rem(xx, SIDE)) * 2 + cc

    def qdev(o, core, axis):
        return dev(y + (1 - axis) * o, x + axis * o, core)

    def pdev(o):
        return dev(y + c * o, x + (1 - c) * o, c)

    def rcopy(src, dst, sid, rid, to):
        return pltpu.make_async_remote_copy(src_ref=src, dst_ref=dst, send_sem=send.at[sid], recv_sem=recv.at[rid], device_id={'ep': to}, device_id_type=MESH)

    sent = []

    def put(src, dst, sid, rid, to):
        cp = rcopy(src, dst, sid, rid, to)
        cp.start()
        sent.append((src, sid))

    def drain(n=None):
        for _ in range(len(sent) if n is None else n):
            src, sid = sent.pop(0)
            rcopy(src, src, sid, 0, me).wait_send()

    def got_it(dst, rid):
        rcopy(dst, dst, 0, rid, me).wait_recv()

    def fetch(src, dst, n):
        cp = pltpu.make_async_copy(src, dst, lsem.at[n])
        cp.start()
        return cp

    lo, hi = pl.ds(0, half), pl.ds(half, half)
    first, last = pl.ds(0, 3 * cap), pl.ds(3 * cap, cap)

    def part(s):
        return pl.ds((0, 1, 3, 2)[s] * cap, cap)

    barrier = pltpu.get_barrier_semaphore()
    peers = [pdev(1), pdev(2), pdev(3), qdev(0, 1 - c, c)]
    peers += [qdev(o, k, c) for o in (1, 3) for k in range(2)]
    peers += [qdev(o, 1 - c, 1 - c) for o in (1, 3)]
    for to in peers:
        pl.semaphore_signal(barrier, inc=1, device_id={'ep': to}, device_id_type=MESH)
    load_hid = fetch(hidh, hid, LHID)
    load_ids = fetch(idsh, idst, LIDS)
    pl.semaphore_wait(barrier, len(peers))

    load_hid.wait()
    put(hid.at[lo], got.at[0, lo], GATHER + 0, GATHER + 0, pdev(1))
    put(hid.at[hi], got.at[2, hi], GATHER + 2, GATHER + 2, pdev(3))
    put(hid.at[hi], got.at[0, hi], GATHER + 1, GATHER + 1, pdev(1))
    put(hid.at[lo], got.at[2, lo], GATHER + 3, GATHER + 3, pdev(3))
    load_rw = fetch(rwh, rw, LRW)
    loads = [fetch(w1h, w1, LW1), fetch(w3h, w3, LW3), fetch(w2h, w2, LW2)]

    load_ids.wait()

    erow = lax.broadcasted_iota(jnp.int32, (experts, tokens), 0)
    hot0, hot1 = idst[0:1, :] == erow, idst[1:2, :] == erow
    one0, one1 = jnp.where(hot0, 1.0, 0.0), jnp.where(hot1, 1.0, 0.0)
    earlier = lax.broadcasted_iota(jnp.int32, (tokens, tokens), 0) < lax.broadcasted_iota(jnp.int32, (tokens, tokens), 1)
    upper = jnp.where(earlier, 1.0, 0.0).astype(bf16)
    before0 = jnp.dot(one0.astype(bf16), upper, preferred_element_type=f32)
    before1 = jnp.dot(one1.astype(bf16), upper, preferred_element_type=f32) + jnp.sum(one0, axis=1, keepdims=True)
    slot0 = jnp.sum(jnp.where(hot0, before0, 0.0), axis=0, keepdims=True)
    slot1 = jnp.sum(jnp.where(hot1, before1, 0.0), axis=0, keepdims=True)
    code[...] = jnp.zeros(code.shape, jnp.int32)
    code[0:1, :] = idst[0:1, :] * cap + slot0.astype(jnp.int32)
    code[1:2, :] = idst[1:2, :] * cap + slot1.astype(jnp.int32)

    order = (2, 1, 3, 0)

    def code_rows(s):
        return code if s == 0 else codes.at[s - 1]

    def slots(o, n=tokens):
        return lax.broadcasted_iota(jnp.int32, (2 * cap, n), 0) + qdev(o, 0, c) * cap

    def pack(s):
        cref = code_rows(s)
        gref = hid if s == 0 else got.at[s - 1]
        c0, c1 = cref[0:1, :], cref[1:2, :]
        for i, o in enumerate(order):
            rows = slots(o)
            pbuf[i * 2 * cap:(i + 1) * 2 * cap, :] = jnp.where((rows == c0) | (rows == c1), 1.0, 0.0).astype(bf16)

        def one(t, carry):
            cols = pl.ds(pl.multiple_of(t * tile, tile), tile)
            r = jnp.dot(pbuf[...], gref[:, cols], preferred_element_type=f32).astype(bf16)
            dst = part(s)
            for i in range(6):
                outq[i, dst, cols] = r[i * cap:(i + 1) * cap]
            r0, r1 = r[6 * cap:7 * cap], r[7 * cap:8 * cap]
            own0 = c == 0
            xs[0, dst, cols] = jnp.where(own0, r0, r1)
            outq[6, dst, cols] = jnp.where(own0, r1, r0)
            return carry

        lax.fori_loop(0, width // tile, one, 0)

    pack(0)
    for s, o in ((1, 1), (3, 3), (2, 2)):
        put(code, codes.at[s - 1], CODE + s - 1, CODE + s - 1, pdev(o))
    got_it(got.at[0, lo], GATHER + 0)
    put(got.at[0, lo], got.at[1, lo], GATHER + 4, GATHER + 4, pdev(1))
    got_it(got.at[2, hi], GATHER + 2)
    put(got.at[2, hi], got.at[1, hi], GATHER + 5, GATHER + 5, pdev(3))

    load_rw.wait()
    w = rw[...]
    wa = w.astype(bf16)
    w = w - wa.astype(f32)
    wb = w.astype(bf16)
    wc = (w - wb.astype(f32)).astype(bf16)
    terms = lax.dot_general(jnp.concatenate([wc, wb, wa], axis=0), hid[...], (((1,), (1,)), ((), ())), preferred_element_type=f32)
    logits = (terms[0:experts] + terms[experts:2 * experts]) + terms[2 * experts:]
    ex = jnp.exp(logits - jnp.max(logits, axis=0, keepdims=True))
    prob = ex / jnp.sum(ex, axis=0, keepdims=True)
    p0 = jnp.sum(jnp.where(hot0, prob, 0.0), axis=0, keepdims=True)
    p1 = jnp.sum(jnp.where(hot1, prob, 0.0), axis=0, keepdims=True)
    gate[0] = jnp.broadcast_to(p0 / (p0 + p1), (128, tokens)).T
    gate[1] = jnp.broadcast_to(p1 / (p0 + p1), (128, tokens)).T

    got_it(codes.at[0], CODE + 0)
    got_it(got.at[0, hi], GATHER + 1)
    pack(1)
    got_it(codes.at[2], CODE + 2)
    got_it(got.at[2, lo], GATHER + 3)
    pack(3)
    put(outq.at[0, first], fwd.at[0, first], LEG + 0, LEG + 0, qdev(1, c, c))
    put(outq.at[1, first], fwd.at[1, first], LEG + 1, LEG + 1, qdev(3, c, c))
    got_it(codes.at[1], CODE + 1)
    got_it(got.at[1, lo], GATHER + 4)
    got_it(got.at[1, hi], GATHER + 5)
    pack(2)

    put(outq.at[0, last], fwd.at[0, last], LEG + 2, LEG + 2, qdev(1, c, c))
    put(outq.at[1, last], fwd.at[1, last], LEG + 3, LEG + 3, qdev(3, c, c))
    put(outq.at[2], xs.at[2 + c], SNBR + 0, CHUNK + 2 + c, qdev(1, 0, c))
    put(outq.at[5], xs.at[2 + c], SNBR + 1, CHUNK + 2 + c, qdev(3, 1, c))
    put(outq.at[6], xs.at[1], CHUNK + 1, CHUNK + 1, qdev(0, 1 - c, c))

    def chunk_forward():
        got_it(fwd.at[0, first], LEG + 0)
        got_it(fwd.at[0, last], LEG + 2)
        put(fwd.at[0], xs.at[4 + c], SFWD + 0, CHUNK + 4 + c, qdev(1, 0, c))
        got_it(fwd.at[1, first], LEG + 1)
        got_it(fwd.at[1, last], LEG + 3)
        put(fwd.at[1], xs.at[4 + c], SFWD + 1, CHUNK + 4 + c, qdev(3, 1, c))
        put(outq.at[3], xs.at[6 + c], SNBR + 2, CHUNK + 6 + c, qdev(1, 1, c))
        put(outq.at[4], xs.at[6 + c], SNBR + 3, CHUNK + 6 + c, qdev(3, 0, c))

    def back_forward(f):
        for i, o in enumerate((1, 3)):
            got_it(bleg.at[i, :, sides[f]], BLEG + 2 * f + i)
            put(bleg.at[i, :, sides[f]], back.at[4 + i, :, sides[f]], SBFWD + 2 * f + i, BACK + 8 * f + 4 + i, qdev(o, c, c))

    def after(step, f):
        k, sid = step % 2, SBACK + 2 * (step - 1)
        if step == 1:
            put(xs.at[1], back.at[c], sid, BACK + c, qdev(0, 1 - c, c))
        elif step in (2, 3):
            put(xs.at[step], back.at[2 + 5 * c], sid, BACK + 2 + 5 * c, qdev(3 + 2 * c, k, k))
        elif step in (4, 5):
            put(xs.at[step, :, sides[f]], bleg.at[c, :, sides[f]], sid + f, BLEG + 2 * f + c, qdev(1 + 2 * c, k, k))
        else:
            put(xs.at[step, :, sides[f]], back.at[6 - 3 * c, :, sides[f]], sid + f, BACK + 8 * f + 6 - 3 * c, qdev(1 + 2 * c, k, k))

    for cp in loads:
        cp.wait()

    def expert(step):
        def up(t, carry):
            cols = pl.ds(pl.multiple_of(t * ftile, ftile), ftile)
            a = jnp.dot(xs[step], w1[:, cols], preferred_element_type=f32)
            b = jnp.dot(xs[step], w3[:, cols], preferred_element_type=f32)
            mid[:, cols] = (jax.nn.silu(a) * b).astype(bf16)
            return carry

        def down(t, carry):
            cols = pl.ds(pl.multiple_of(t * tile, tile), tile)
            r = jnp.dot(mid[...], w2[:, cols], preferred_element_type=f32).astype(bf16)
            if step == 0:
                back[c, :, cols] = r
            else:
                xs[step, :, cols] = r
            return carry

        lax.fori_loop(0, ffn // ftile, up, 0)
        if step == 7:
            back_forward(1)
        tiles = width // tile
        if step < 4:
            lax.fori_loop(0, tiles, down, 0)
            if step:
                after(step, 0)
        else:
            lax.fori_loop(0, tiles // 2, down, 0)
            after(step, 0)
            lax.fori_loop(tiles // 2, tiles, down, 0)
            after(step, 1)

    for step in range(8):
        if step:
            got_it(xs.at[step], CHUNK + step)
        expert(step)
        if step == 1:
            chunk_forward()
            chunks_sent = len(sent)
        elif step == 6:
            back_forward(0)

    drain(chunks_sent)

    def place(s, k, dst, f):
        ck = code_rows(s)[k:k + 1, :]
        for o in range(SIDE):
            pbuf[o * 2 * cap:(o + 1) * 2 * cap, :] = jnp.where(slots(o) == ck, 1.0, 0.0).astype(bf16)

        def one(t, carry):
            cols = pl.ds(pl.multiple_of(f * wide + t * tile, tile), tile)
            rows = back[:, part(s), cols].reshape(8 * cap, tile)
            dst[:, cols] = lax.dot_general(pbuf[...], rows, (((0,), (0,)), ((), ())), preferred_element_type=f32).astype(bf16)
            return carry

        lax.fori_loop(0, wide // tile, one, 0)

    def unmerged(f):
        h = sides[f]
        for i, (k, o) in enumerate(((0, 1), (1, 3))):
            place(2, k, outq.at[i], f)
            put(outq.at[i, :, h], lbuf.at[i, :, h], HOPP + 2 * f + i, HOPP + 2 * f + i, pdev(o))
        for i, (s, k, o) in enumerate(((3, 1, 1), (1, 0, 3))):
            place(s, k, outq.at[2 + i], f)
            put(outq.at[2 + i, :, h], rbuf.at[1 + i, :, h], HOME + 2 * f + i, HOME + 2 * f + i, pdev(o))

    def mergeable(f):
        place(3, 0, outq.at[4], f)
        place(1, 1, outq.at[5], f)

    def merged(f):
        h = sides[f]
        for i, o in enumerate((1, 3)):
            got_it(lbuf.at[i, :, h], HOPP + 2 * f + i)
            outq[4 + i, :, h] = outq[4 + i, :, h] + lbuf[i, :, h]
            put(outq.at[4 + i, :, h], rbuf.at[3 * i, :, h], HOME + 4 + 2 * f + i, HOME + 4 + 2 * f + i, pdev(o))

    got_it(back.at[1 - c], BACK + 1 - c)
    for blk in (2, 7):
        got_it(back.at[blk], BACK + blk)
    for f in range(2):
        for blk in (3, 6, 4, 5):
            got_it(back.at[blk, :, sides[f]], BACK + 8 * f + blk)
        unmerged(f)
        if f == 0:
            mergeable(0)
    merged(0)
    mergeable(1)
    merged(1)
    for k in range(2):
        for f in range(2):
            place(0, k, got.at[k], f)
    step_rows = min(64, tokens)
    outs = []
    for f in range(2):
        h = sides[f]
        for i in range(2):
            got_it(rbuf.at[1 + i, :, h], HOME + 2 * f + i)
        for i in range(2):
            got_it(rbuf.at[3 * i, :, h], HOME + 4 + 2 * f + i)

        def finish(j, carry):
            r = pl.ds(pl.multiple_of(j * step_rows, step_rows), step_rows)
            g0, g1 = gate[0, r, 0:1], gate[1, r, 0:1]
            for t in range(wide // tile):
                cols = pl.ds(f * wide + t * tile, tile)
                y0 = (got[0, r, cols] + rbuf[0, r, cols] + rbuf[2, r, cols]).astype(f32)
                y1 = (got[1, r, cols] + rbuf[1, r, cols] + rbuf[3, r, cols]).astype(f32)
                mixed = g0 * y0 + g1 * y1
                outq[6, r, cols] = (scale[0] * hid[r, cols].astype(f32) + scale[1] * mixed).astype(bf16)
            return carry

        lax.fori_loop(0, tokens // step_rows, finish, 0)
        outs.append(fetch(outq.at[6, :, h], out.at[:, h], LOUT + f))
    drain()
    for cp in outs:
        cp.wait()


def fused(hidden, rw, idst, scale, w1, w3, w2, cap):
    tokens, width = hidden.shape
    ffn = w1.shape[1]
    rows = SIDE * cap
    bf = jnp.bfloat16
    hbm = pl.BlockSpec(memory_space=pl.ANY)
    return pl.pallas_call(
        kernel_body,
        out_shape=[
            jax.ShapeDtypeStruct((tokens, width), bf),
            jax.ShapeDtypeStruct((2, rows, width), bf),
            jax.ShapeDtypeStruct((2, rows, width), bf),
        ],
        in_specs=[hbm, pl.BlockSpec(memory_space=pltpu.SMEM), hbm, hbm, hbm, hbm, hbm],
        out_specs=[hbm, hbm, hbm],
        scratch_shapes=[
            pltpu.VMEM(idst.shape, jnp.int32),
            pltpu.VMEM((tokens, width), bf),
            pltpu.VMEM(rw.shape, jnp.float32),
            pltpu.VMEM((width, ffn), bf), pltpu.VMEM((width, ffn), bf), pltpu.VMEM((ffn, width), bf),
            pltpu.VMEM((3, tokens, width), bf),
            pltpu.VMEM((8, tokens), jnp.int32),
            pltpu.VMEM((3, 8, tokens), jnp.int32),
            pltpu.VMEM((2, tokens, 128), jnp.float32),
            pltpu.VMEM((8 * cap, tokens), bf),
            pltpu.VMEM((8, rows, width), bf),
            pltpu.VMEM((7, rows, width), bf),
            pltpu.VMEM((rows, ffn), bf),
            pltpu.VMEM((8, rows, width), bf),
            pltpu.VMEM((2, tokens, width), bf),
            pltpu.VMEM((4, tokens, width), bf),
            pltpu.SemaphoreType.DMA((NSEND,)),
            pltpu.SemaphoreType.DMA((NMSG,)),
            pltpu.SemaphoreType.DMA((8,)),
        ],
        compiler_params=pltpu.CompilerParams(has_side_effects=True, collective_id=0, vmem_limit_bytes=67043328),
        name='moe',
    )(idst, scale, hidden, rw, w1, w3, w2)[0]


def solution(mesh):
    ep_size = mesh.shape['ep']

    def local_step(hidden, router_w, expert_ids, w_gate, w_up, w_down, post_scale):
        tokens = hidden.shape[0]
        experts = w_gate.shape[0] * ep_size
        cap = tokens // max(1, experts // 8)
        out = fused(hidden, router_w.T, expert_ids.T, post_scale, w_gate[0], w_up[0], w_down[0], cap)
        return jnp.where(jnp.isnan(out), jnp.nan, out)

    tok_spec = P(('dp', 'ep'))
    return jax.shard_map(local_step, mesh=mesh, in_specs=(tok_spec, P(), tok_spec, P('ep'), P('ep'), P('ep'), P()), out_specs=tok_spec, check_vma=False)
```

```python
import functools
import jax
import jax.numpy as jnp
from jax import lax
from jax.experimental import pallas as pl
from jax.experimental.pallas import tpu as pltpu
from jax.sharding import PartitionSpec as P

MESH = pl.DeviceIdType.MESH
SIDE = 4

CODE = 0
GATHER = 3
CHUNK = 9
LEG = 17
BACK = 21
BLEG = 37
HOPP = 41
HOME = 45
NMSG = 57
SFWD = 57
SBFWD = 59
SNBR = 63
SBACK = 67
NSEND = 81
LHID, LRW, LW1, LW3, LW2, LOUT, LIDS = 0, 1, 2, 3, 4, 5, 7


def kernel_body(idsh, scale, hidh, rwh, w1h, w3h, w2h,
                out, fwd, bleg,
                idst, hid, rw, w1, w3, w2, got, code, codes, gate, pbuf, xs, outq, mid, back, lbuf, rbuf,
                send, recv, lsem):
    tokens, width = hid.shape
    cap = xs.shape[1] // SIDE
    ffn = w1.shape[1]
    experts = rw.shape[0]
    half = tokens // 2
    tile = min(512, width // 2)
    wide = width // 2
    sides = (pl.ds(0, wide), pl.ds(wide, wide))
    ftile = min(512, ffn)
    f32, bf16 = jnp.float32, jnp.bfloat16
    me = lax.axis_index('ep')
    y, x, c = lax.div(me, 2 * SIDE), lax.rem(lax.div(me, 2), SIDE), lax.rem(me, 2)

    def dev(yy, xx, cc):
        return (lax.rem(yy, SIDE) * SIDE + lax.rem(xx, SIDE)) * 2 + cc

    def qdev(o, core, axis):
        return dev(y + (1 - axis) * o, x + axis * o, core)

    def pdev(o):
        return dev(y + c * o, x + (1 - c) * o, c)

    def rcopy(src, dst, sid, rid, to):
        return pltpu.make_async_remote_copy(src_ref=src, dst_ref=dst, send_sem=send.at[sid], recv_sem=recv.at[rid], device_id={'ep': to}, device_id_type=MESH)

    sent = []

    def put(src, dst, sid, rid, to):
        cp = rcopy(src, dst, sid, rid, to)
        cp.start()
        sent.append((src, sid))

    def drain(n=None):
        for _ in range(len(sent) if n is None else n):
            src, sid = sent.pop(0)
            rcopy(src, src, sid, 0, me).wait_send()

    def got_it(dst, rid):
        rcopy(dst, dst, 0, rid, me).wait_recv()

    def fetch(src, dst, n):
        cp = pltpu.make_async_copy(src, dst, lsem.at[n])
        cp.start()
        return cp

    lo, hi = pl.ds(0, half), pl.ds(half, half)
    first, last = pl.ds(0, 3 * cap), pl.ds(3 * cap, cap)

    def part(s):
        return pl.ds((0, 1, 3, 2)[s] * cap, cap)

    barrier = pltpu.get_barrier_semaphore()
    peers = [pdev(1), pdev(2), pdev(3), qdev(0, 1 - c, c)]
    peers += [qdev(o, k, c) for o in (1, 3) for k in range(2)]
    peers += [qdev(o, 1 - c, 1 - c) for o in (1, 3)]
    for to in peers:
        pl.semaphore_signal(barrier, inc=1, device_id={'ep': to}, device_id_type=MESH)
    load_hid = fetch(hidh, hid, LHID)
    load_ids = fetch(idsh, idst, LIDS)
    pl.semaphore_wait(barrier, len(peers))

    load_hid.wait()
    put(hid.at[lo], got.at[0, lo], GATHER + 0, GATHER + 0, pdev(1))
    put(hid.at[hi], got.at[2, hi], GATHER + 2, GATHER + 2, pdev(3))
    put(hid.at[hi], got.at[0, hi], GATHER + 1, GATHER + 1, pdev(1))
    put(hid.at[lo], got.at[2, lo], GATHER + 3, GATHER + 3, pdev(3))
    load_rw = fetch(rwh, rw, LRW)
    loads = [fetch(w1h, w1, LW1), fetch(w3h, w3, LW3), fetch(w2h, w2, LW2)]

    load_ids.wait()

    erow = lax.broadcasted_iota(jnp.int32, (experts, tokens), 0)
    hot0, hot1 = idst[0:1, :] == erow, idst[1:2, :] == erow
    one0, one1 = jnp.where(hot0, 1.0, 0.0), jnp.where(hot1, 1.0, 0.0)
    earlier = lax.broadcasted_iota(jnp.int32, (tokens, tokens), 0) < lax.broadcasted_iota(jnp.int32, (tokens, tokens), 1)
    upper = jnp.where(earlier, 1.0, 0.0).astype(bf16)
    before0 = jnp.dot(one0.astype(bf16), upper, preferred_element_type=f32)
    before1 = jnp.dot(one1.astype(bf16), upper, preferred_element_type=f32) + jnp.sum(one0, axis=1, keepdims=True)
    slot0 = jnp.sum(jnp.where(hot0, before0, 0.0), axis=0, keepdims=True)
    slot1 = jnp.sum(jnp.where(hot1, before1, 0.0), axis=0, keepdims=True)
    code[...] = jnp.zeros(code.shape, jnp.int32)
    code[0:1, :] = idst[0:1, :] * cap + slot0.astype(jnp.int32)
    code[1:2, :] = idst[1:2, :] * cap + slot1.astype(jnp.int32)

    order = (2, 1, 3, 0)

    def code_rows(s):
        return code if s == 0 else codes.at[s - 1]

    def slots(o, n=tokens):
        return lax.broadcasted_iota(jnp.int32, (2 * cap, n), 0) + qdev(o, 0, c) * cap

    def pack(s):
        cref = code_rows(s)
        gref = hid if s == 0 else got.at[s - 1]
        c0, c1 = cref[0:1, :], cref[1:2, :]
        for i, o in enumerate(order):
            rows = slots(o)
            pbuf[i * 2 * cap:(i + 1) * 2 * cap, :] = jnp.where((rows == c0) | (rows == c1), 1.0, 0.0).astype(bf16)

        def one(t, carry):
            cols = pl.ds(pl.multiple_of(t * tile, tile), tile)
            r = jnp.dot(pbuf[...], gref[:, cols], preferred_element_type=f32).astype(bf16)
            dst = part(s)
            for i in range(6):
                outq[i, dst, cols] = r[i * cap:(i + 1) * cap]
            r0, r1 = r[6 * cap:7 * cap], r[7 * cap:8 * cap]
            own0 = c == 0
            xs[0, dst, cols] = jnp.where(own0, r0, r1)
            outq[6, dst, cols] = jnp.where(own0, r1, r0)
            return carry

        lax.fori_loop(0, width // tile, one, 0)

    pack(0)
    for s, o in ((1, 1), (3, 3), (2, 2)):
        put(code, codes.at[s - 1], CODE + s - 1, CODE + s - 1, pdev(o))
    got_it(got.at[0, lo], GATHER + 0)
    put(got.at[0, lo], got.at[1, lo], GATHER + 4, GATHER + 4, pdev(1))
    got_it(got.at[2, hi], GATHER + 2)
    put(got.at[2, hi], got.at[1, hi], GATHER + 5, GATHER + 5, pdev(3))

    load_rw.wait()
    w = rw[...]
    wa = w.astype(bf16)
    w = w - wa.astype(f32)
    wb = w.astype(bf16)
    wc = (w - wb.astype(f32)).astype(bf16)
    terms = lax.dot_general(jnp.concatenate([wc, wb, wa], axis=0), hid[...], (((1,), (1,)), ((), ())), preferred_element_type=f32)
    logits = (terms[0:experts] + terms[experts:2 * experts]) + terms[2 * experts:]
    ex = jnp.exp(logits - jnp.max(logits, axis=0, keepdims=True))
    prob = ex / jnp.sum(ex, axis=0, keepdims=True)
    p0 = jnp.sum(jnp.where(hot0, prob, 0.0), axis=0, keepdims=True)
    p1 = jnp.sum(jnp.where(hot1, prob, 0.0), axis=0, keepdims=True)
    gate[0] = jnp.broadcast_to(p0 / (p0 + p1), (128, tokens)).T
    gate[1] = jnp.broadcast_to(p1 / (p0 + p1), (128, tokens)).T

    got_it(codes.at[0], CODE + 0)
    got_it(got.at[0, hi], GATHER + 1)
    pack(1)
    got_it(codes.at[2], CODE + 2)
    got_it(got.at[2, lo], GATHER + 3)
    pack(3)
    put(outq.at[0, first], fwd.at[0, first], LEG + 0, LEG + 0, qdev(1, c, c))
    put(outq.at[1, first], fwd.at[1, first], LEG + 1, LEG + 1, qdev(3, c, c))
    got_it(codes.at[1], CODE + 1)
    got_it(got.at[1, lo], GATHER + 4)
    got_it(got.at[1, hi], GATHER + 5)
    pack(2)

    put(outq.at[0, last], fwd.at[0, last], LEG + 2, LEG + 2, qdev(1, c, c))
    put(outq.at[1, last], fwd.at[1, last], LEG + 3, LEG + 3, qdev(3, c, c))
    put(outq.at[2], xs.at[2 + c], SNBR + 0, CHUNK + 2 + c, qdev(1, 0, c))
    put(outq.at[5], xs.at[2 + c], SNBR + 1, CHUNK + 2 + c, qdev(3, 1, c))
    put(outq.at[6], xs.at[1], CHUNK + 1, CHUNK + 1, qdev(0, 1 - c, c))

    def chunk_forward():
        got_it(fwd.at[0, first], LEG + 0)
        got_it(fwd.at[0, last], LEG + 2)
        put(fwd.at[0], xs.at[4 + c], SFWD + 0, CHUNK + 4 + c, qdev(1, 0, c))
        got_it(fwd.at[1, first], LEG + 1)
        got_it(fwd.at[1, last], LEG + 3)
        put(fwd.at[1], xs.at[4 + c], SFWD + 1, CHUNK + 4 + c, qdev(3, 1, c))
        put(outq.at[3], xs.at[6 + c], SNBR + 2, CHUNK + 6 + c, qdev(1, 1, c))
        put(outq.at[4], xs.at[6 + c], SNBR + 3, CHUNK + 6 + c, qdev(3, 0, c))

    def back_forward(f):
        for i, o in enumerate((1, 3)):
            got_it(bleg.at[i, :, sides[f]], BLEG + 2 * f + i)
            put(bleg.at[i, :, sides[f]], back.at[4 + i, :, sides[f]], SBFWD + 2 * f + i, BACK + 8 * f + 4 + i, qdev(o, c, c))

    def after(step, f):
        k, sid = step % 2, SBACK + 2 * (step - 1)
        if step == 1:
            put(xs.at[1], back.at[c], sid, BACK + c, qdev(0, 1 - c, c))
        elif step in (2, 3):
            put(xs.at[step], back.at[2 + 5 * c], sid, BACK + 2 + 5 * c, qdev(3 + 2 * c, k, k))
        elif step in (4, 5):
            put(xs.at[step, :, sides[f]], bleg.at[c, :, sides[f]], sid + f, BLEG + 2 * f + c, qdev(1 + 2 * c, k, k))
        else:
            put(xs.at[step, :, sides[f]], back.at[6 - 3 * c, :, sides[f]], sid + f, BACK + 8 * f + 6 - 3 * c, qdev(1 + 2 * c, k, k))

    for cp in loads:
        cp.wait()

    def expert(step):
        def up(t, carry):
            cols = pl.ds(pl.multiple_of(t * ftile, ftile), ftile)
            a = jnp.dot(xs[step], w1[:, cols], preferred_element_type=f32)
            b = jnp.dot(xs[step], w3[:, cols], preferred_element_type=f32)
            mid[:, cols] = (jax.nn.silu(a) * b).astype(bf16)
            return carry

        def down(t, carry):
            cols = pl.ds(pl.multiple_of(t * tile, tile), tile)
            r = jnp.dot(mid[...], w2[:, cols], preferred_element_type=f32).astype(bf16)
            if step == 0:
                back[c, :, cols] = r
            else:
                xs[step, :, cols] = r
            return carry

        lax.fori_loop(0, ffn // ftile, up, 0)
        if step == 7:
            back_forward(1)
        tiles = width // tile
        if step < 4:
            lax.fori_loop(0, tiles, down, 0)
            if step:
                after(step, 0)
        else:
            lax.fori_loop(0, tiles // 2, down, 0)
            after(step, 0)
            lax.fori_loop(tiles // 2, tiles, down, 0)
            after(step, 1)

    for step in range(8):
        if step:
            got_it(xs.at[step], CHUNK + step)
        expert(step)
        if step == 1:
            chunk_forward()
            chunks_sent = len(sent)
        elif step == 6:
            back_forward(0)

    drain(chunks_sent)

    def place(s, k, dst, f):
        ck = code_rows(s)[k:k + 1, :]
        for o in range(SIDE):
            pbuf[o * 2 * cap:(o + 1) * 2 * cap, :] = jnp.where(slots(o) == ck, 1.0, 0.0).astype(bf16)

        def one(t, carry):
            cols = pl.ds(pl.multiple_of(f * wide + t * tile, tile), tile)
            rows = back[:, part(s), cols].reshape(8 * cap, tile)
            dst[:, cols] = lax.dot_general(pbuf[...], rows, (((0,), (0,)), ((), ())), preferred_element_type=f32).astype(bf16)
            return carry

        lax.fori_loop(0, wide // tile, one, 0)

    def unmerged(f):
        h = sides[f]
        for i, (k, o) in enumerate(((0, 1), (1, 3))):
            place(2, k, outq.at[i], f)
            put(outq.at[i, :, h], lbuf.at[i, :, h], HOPP + 2 * f + i, HOPP + 2 * f + i, pdev(o))
        for i, (s, k, o) in enumerate(((3, 1, 1), (1, 0, 3))):
            place(s, k, outq.at[2 + i], f)
            put(outq.at[2 + i, :, h], rbuf.at[1 + i, :, h], HOME + 2 * f + i, HOME + 2 * f + i, pdev(o))

    def mergeable(f):
        place(3, 0, outq.at[4], f)
        place(1, 1, outq.at[5], f)

    def merged(f):
        h = sides[f]
        for i, o in enumerate((1, 3)):
            got_it(lbuf.at[i, :, h], HOPP + 2 * f + i)
            for j, r in enumerate((lo, hi)):
                sid = HOME + 4 + 4 * f + 2 * i + j
                outq[4 + i, r, h] = outq[4 + i, r, h] + lbuf[i, r, h]
                put(outq.at[4 + i, r, h], rbuf.at[3 * i, r, h], sid, sid, pdev(o))

    got_it(back.at[1 - c], BACK + 1 - c)
    for blk in (2, 7):
        got_it(back.at[blk], BACK + blk)
    for f in range(2):
        for blk in (3, 6, 4, 5):
            got_it(back.at[blk, :, sides[f]], BACK + 8 * f + blk)
        unmerged(f)
        if f == 0:
            mergeable(0)
    merged(0)
    mergeable(1)
    merged(1)
    for k in range(2):
        for f in range(2):
            place(0, k, got.at[k], f)
    step_rows = min(64, half)
    for f in range(2):
        h = sides[f]
        for i in range(2):
            got_it(rbuf.at[1 + i, :, h], HOME + 2 * f + i)
        for m, part_rows in enumerate((lo, hi)):
            for i in range(2):
                got_it(rbuf.at[3 * i, part_rows, h], HOME + 4 + 4 * f + 2 * i + m)

            def finish(j, carry):
                r = pl.ds(pl.multiple_of(m * half + j * step_rows, step_rows), step_rows)
                g0, g1 = gate[0, r, 0:1], gate[1, r, 0:1]
                for t in range(wide // tile):
                    cols = pl.ds(f * wide + t * tile, tile)
                    y0 = (got[0, r, cols] + rbuf[0, r, cols] + rbuf[2, r, cols]).astype(f32)
                    y1 = (got[1, r, cols] + rbuf[1, r, cols] + rbuf[3, r, cols]).astype(f32)
                    mixed = g0 * y0 + g1 * y1
                    out[r, cols] = (scale[0] * hid[r, cols].astype(f32) + scale[1] * mixed).astype(bf16)
                return carry

            lax.fori_loop(0, half // step_rows, finish, 0)
    drain()


def fused(hidden, rw, idst, scale, w1, w3, w2, cap):
    tokens, width = hidden.shape
    ffn = w1.shape[1]
    rows = SIDE * cap
    bf = jnp.bfloat16
    hbm = pl.BlockSpec(memory_space=pl.ANY)
    return pl.pallas_call(
        kernel_body,
        out_shape=[
            pltpu.VMEM((tokens, width), bf),
            jax.ShapeDtypeStruct((2, rows, width), bf),
            jax.ShapeDtypeStruct((2, rows, width), bf),
        ],
        in_specs=[hbm, pl.BlockSpec(memory_space=pltpu.SMEM), hbm, hbm, hbm, hbm, hbm],
        out_specs=[pl.BlockSpec(memory_space=pltpu.VMEM), hbm, hbm],
        scratch_shapes=[
            pltpu.VMEM(idst.shape, jnp.int32),
            pltpu.VMEM((tokens, width), bf),
            pltpu.VMEM(rw.shape, jnp.float32),
            pltpu.VMEM((width, ffn), bf), pltpu.VMEM((width, ffn), bf), pltpu.VMEM((ffn, width), bf),
            pltpu.VMEM((3, tokens, width), bf),
            pltpu.VMEM((8, tokens), jnp.int32),
            pltpu.VMEM((3, 8, tokens), jnp.int32),
            pltpu.VMEM((2, tokens, 128), jnp.float32),
            pltpu.VMEM((8 * cap, tokens), bf),
            pltpu.VMEM((8, rows, width), bf),
            pltpu.VMEM((7, rows, width), bf),
            pltpu.VMEM((rows, ffn), bf),
            pltpu.VMEM((8, rows, width), bf),
            pltpu.VMEM((2, tokens, width), bf),
            pltpu.VMEM((4, tokens, width), bf),
            pltpu.SemaphoreType.DMA((NSEND,)),
            pltpu.SemaphoreType.DMA((NMSG,)),
            pltpu.SemaphoreType.DMA((8,)),
        ],
        compiler_params=pltpu.CompilerParams(has_side_effects=True, collective_id=0, vmem_limit_bytes=64000000),
        name='moe',
    )(idst, scale, hidden, rw, w1, w3, w2)[0]


def solution(mesh):
    ep_size = mesh.shape['ep']

    def local_step(hidden, router_w, expert_ids, w_gate, w_up, w_down, post_scale):
        tokens = hidden.shape[0]
        experts = w_gate.shape[0] * ep_size
        cap = tokens // max(1, experts // 8)
        out = fused(hidden, router_w.T, expert_ids.T, post_scale, w_gate[0], w_up[0], w_down[0], cap)
        return out

    tok_spec = P(('dp', 'ep'))
    return jax.shard_map(local_step, mesh=mesh, in_specs=(tok_spec, P(), tok_spec, P('ep'), P('ep'), P('ep'), P()), out_specs=tok_spec, check_vma=False)
```

```python
import functools
import jax
import jax.numpy as jnp
from jax import lax
from jax.experimental import pallas as pl
from jax.experimental.pallas import tpu as pltpu
from jax.sharding import PartitionSpec as P

MESH = pl.DeviceIdType.MESH
SIDE = 4

CODE = 0
GATHER = 3
CHUNK = 9
LEG = 17
BACK = 21
BLEG = 37
HOPP = 41
HOME = 45
NMSG = 57
SFWD = 57
SBFWD = 59
SNBR = 63
SBACK = 67
NSEND = 81
LHID, LRW, LW1, LW3, LW2, LOUT, LIDS = 0, 1, 2, 3, 4, 5, 7


def kernel_body(idsh, scale, hidh, rwh, w1h, w3h, w2h,
                out, fwd,
                idst, hid, rw, w1, w3, w2, got, code, codes, gate, pbuf, xs, outq, mid, back, bleg, lbuf, rbuf,
                send, recv, lsem):
    tokens, width = hid.shape
    cap = xs.shape[1] // SIDE
    ffn = w1.shape[1]
    experts = rw.shape[0]
    half = tokens // 2
    tile = min(512, width // 2)
    wide = width // 2
    sides = (pl.ds(0, wide), pl.ds(wide, wide))
    ftile = min(512, ffn)
    f32, bf16 = jnp.float32, jnp.bfloat16
    me = lax.axis_index('ep')
    y, x, c = lax.div(me, 2 * SIDE), lax.rem(lax.div(me, 2), SIDE), lax.rem(me, 2)

    def dev(yy, xx, cc):
        return (lax.rem(yy, SIDE) * SIDE + lax.rem(xx, SIDE)) * 2 + cc

    def qdev(o, core, axis):
        return dev(y + (1 - axis) * o, x + axis * o, core)

    def pdev(o):
        return dev(y + c * o, x + (1 - c) * o, c)

    def rcopy(src, dst, sid, rid, to):
        return pltpu.make_async_remote_copy(src_ref=src, dst_ref=dst, send_sem=send.at[sid], recv_sem=recv.at[rid], device_id={'ep': to}, device_id_type=MESH)

    sent = []

    def put(src, dst, sid, rid, to):
        cp = rcopy(src, dst, sid, rid, to)
        cp.start()
        sent.append((src, sid))

    def drain(n=None):
        for _ in range(len(sent) if n is None else n):
            src, sid = sent.pop(0)
            rcopy(src, src, sid, 0, me).wait_send()

    def got_it(dst, rid):
        rcopy(dst, dst, 0, rid, me).wait_recv()

    def fetch(src, dst, n):
        cp = pltpu.make_async_copy(src, dst, lsem.at[n])
        cp.start()
        return cp

    lo, hi = pl.ds(0, half), pl.ds(half, half)
    first, last = pl.ds(0, 3 * cap), pl.ds(3 * cap, cap)

    def part(s):
        return pl.ds((0, 1, 3, 2)[s] * cap, cap)

    barrier = pltpu.get_barrier_semaphore()
    peers = [pdev(1), pdev(2), pdev(3), qdev(0, 1 - c, c)]
    peers += [qdev(o, k, c) for o in (1, 3) for k in range(2)]
    peers += [qdev(o, 1 - c, 1 - c) for o in (1, 3)]
    for to in peers:
        pl.semaphore_signal(barrier, inc=1, device_id={'ep': to}, device_id_type=MESH)
    load_hid = fetch(hidh, hid, LHID)
    load_ids = fetch(idsh, idst, LIDS)
    pl.semaphore_wait(barrier, len(peers))

    load_hid.wait()
    put(hid.at[lo], got.at[0, lo], GATHER + 0, GATHER + 0, pdev(1))
    put(hid.at[hi], got.at[2, hi], GATHER + 2, GATHER + 2, pdev(3))
    put(hid.at[hi], got.at[0, hi], GATHER + 1, GATHER + 1, pdev(1))
    put(hid.at[lo], got.at[2, lo], GATHER + 3, GATHER + 3, pdev(3))
    load_rw = fetch(rwh, rw, LRW)
    loads = [fetch(w1h, w1, LW1), fetch(w3h, w3, LW3), fetch(w2h, w2, LW2)]

    load_ids.wait()

    erow = lax.broadcasted_iota(jnp.int32, (experts, tokens), 0)
    hot0, hot1 = idst[0:1, :] == erow, idst[1:2, :] == erow
    one0, one1 = jnp.where(hot0, 1.0, 0.0), jnp.where(hot1, 1.0, 0.0)
    earlier = lax.broadcasted_iota(jnp.int32, (tokens, tokens), 0) < lax.broadcasted_iota(jnp.int32, (tokens, tokens), 1)
    upper = jnp.where(earlier, 1.0, 0.0).astype(bf16)
    before0 = jnp.dot(one0.astype(bf16), upper, preferred_element_type=f32)
    before1 = jnp.dot(one1.astype(bf16), upper, preferred_element_type=f32) + jnp.sum(one0, axis=1, keepdims=True)
    slot0 = jnp.sum(jnp.where(hot0, before0, 0.0), axis=0, keepdims=True)
    slot1 = jnp.sum(jnp.where(hot1, before1, 0.0), axis=0, keepdims=True)
    code[...] = jnp.zeros(code.shape, jnp.int32)
    code[0:1, :] = idst[0:1, :] * cap + slot0.astype(jnp.int32)
    code[1:2, :] = idst[1:2, :] * cap + slot1.astype(jnp.int32)

    order = (2, 1, 3, 0)

    def code_rows(s):
        return code if s == 0 else codes.at[s - 1]

    def slots(o, n=tokens):
        return lax.broadcasted_iota(jnp.int32, (2 * cap, n), 0) + qdev(o, 0, c) * cap

    def pack(s):
        cref = code_rows(s)
        gref = hid if s == 0 else got.at[s - 1]
        c0, c1 = cref[0:1, :], cref[1:2, :]
        for i, o in enumerate(order):
            rows = slots(o)
            pbuf[i * 2 * cap:(i + 1) * 2 * cap, :] = jnp.where((rows == c0) | (rows == c1), 1.0, 0.0).astype(bf16)

        def one(t, carry):
            cols = pl.ds(pl.multiple_of(t * tile, tile), tile)
            r = jnp.dot(pbuf[...], gref[:, cols], preferred_element_type=f32).astype(bf16)
            dst = part(s)
            for i in range(6):
                outq[i, dst, cols] = r[i * cap:(i + 1) * cap]
            r0, r1 = r[6 * cap:7 * cap], r[7 * cap:8 * cap]
            own0 = c == 0
            xs[0, dst, cols] = jnp.where(own0, r0, r1)
            outq[6, dst, cols] = jnp.where(own0, r1, r0)
            return carry

        lax.fori_loop(0, width // tile, one, 0)

    pack(0)
    for s, o in ((1, 1), (3, 3), (2, 2)):
        put(code, codes.at[s - 1], CODE + s - 1, CODE + s - 1, pdev(o))
    got_it(got.at[0, lo], GATHER + 0)
    put(got.at[0, lo], got.at[1, lo], GATHER + 4, GATHER + 4, pdev(1))
    got_it(got.at[2, hi], GATHER + 2)
    put(got.at[2, hi], got.at[1, hi], GATHER + 5, GATHER + 5, pdev(3))

    load_rw.wait()
    w = rw[...]
    wa = w.astype(bf16)
    w = w - wa.astype(f32)
    wb = w.astype(bf16)
    wc = (w - wb.astype(f32)).astype(bf16)
    terms = lax.dot_general(jnp.concatenate([wc, wb, wa], axis=0), hid[...], (((1,), (1,)), ((), ())), preferred_element_type=f32)
    logits = (terms[0:experts] + terms[experts:2 * experts]) + terms[2 * experts:]
    ex = jnp.exp(logits - jnp.max(logits, axis=0, keepdims=True))
    prob = ex / jnp.sum(ex, axis=0, keepdims=True)
    p0 = jnp.sum(jnp.where(hot0, prob, 0.0), axis=0, keepdims=True)
    p1 = jnp.sum(jnp.where(hot1, prob, 0.0), axis=0, keepdims=True)
    gate[0] = jnp.broadcast_to(p0 / (p0 + p1), (128, tokens)).T
    gate[1] = jnp.broadcast_to(p1 / (p0 + p1), (128, tokens)).T

    got_it(codes.at[0], CODE + 0)
    got_it(got.at[0, hi], GATHER + 1)
    pack(1)
    got_it(codes.at[2], CODE + 2)
    got_it(got.at[2, lo], GATHER + 3)
    pack(3)
    put(outq.at[0, first], fwd.at[0, first], LEG + 0, LEG + 0, qdev(1, c, c))
    put(outq.at[1, first], fwd.at[1, first], LEG + 1, LEG + 1, qdev(3, c, c))
    got_it(codes.at[1], CODE + 1)
    got_it(got.at[1, lo], GATHER + 4)
    got_it(got.at[1, hi], GATHER + 5)
    pack(2)

    put(outq.at[0, last], fwd.at[0, last], LEG + 2, LEG + 2, qdev(1, c, c))
    put(outq.at[1, last], fwd.at[1, last], LEG + 3, LEG + 3, qdev(3, c, c))
    put(outq.at[2], xs.at[2 + c], SNBR + 0, CHUNK + 2 + c, qdev(1, 0, c))
    put(outq.at[5], xs.at[2 + c], SNBR + 1, CHUNK + 2 + c, qdev(3, 1, c))
    put(outq.at[6], xs.at[1], CHUNK + 1, CHUNK + 1, qdev(0, 1 - c, c))

    def chunk_forward():
        got_it(fwd.at[0, first], LEG + 0)
        got_it(fwd.at[0, last], LEG + 2)
        put(fwd.at[0], xs.at[4 + c], SFWD + 0, CHUNK + 4 + c, qdev(1, 0, c))
        got_it(fwd.at[1, first], LEG + 1)
        got_it(fwd.at[1, last], LEG + 3)
        put(fwd.at[1], xs.at[4 + c], SFWD + 1, CHUNK + 4 + c, qdev(3, 1, c))
        put(outq.at[3], xs.at[6 + c], SNBR + 2, CHUNK + 6 + c, qdev(1, 1, c))
        put(outq.at[4], xs.at[6 + c], SNBR + 3, CHUNK + 6 + c, qdev(3, 0, c))

    def back_forward(f):
        for i, o in enumerate((1, 3)):
            got_it(bleg.at[i, :, sides[f]], BLEG + 2 * f + i)
            put(bleg.at[i, :, sides[f]], back.at[4 + i, :, sides[f]], SBFWD + 2 * f + i, BACK + 8 * f + 4 + i, qdev(o, c, c))

    def after(step, f):
        k, sid = step % 2, SBACK + 2 * (step - 1)
        if step == 1:
            put(xs.at[1], back.at[c], sid, BACK + c, qdev(0, 1 - c, c))
        elif step in (2, 3):
            put(xs.at[step], back.at[2 + 5 * c], sid, BACK + 2 + 5 * c, qdev(3 + 2 * c, k, k))
        elif step in (4, 5):
            put(xs.at[step, :, sides[f]], bleg.at[c, :, sides[f]], sid + f, BLEG + 2 * f + c, qdev(1 + 2 * c, k, k))
        else:
            put(xs.at[step, :, sides[f]], back.at[6 - 3 * c, :, sides[f]], sid + f, BACK + 8 * f + 6 - 3 * c, qdev(1 + 2 * c, k, k))

    for cp in loads:
        cp.wait()

    def expert(step):
        def up(t, carry):
            cols = pl.ds(pl.multiple_of(t * ftile, ftile), ftile)
            a = jnp.dot(xs[step], w1[:, cols], preferred_element_type=f32)
            b = jnp.dot(xs[step], w3[:, cols], preferred_element_type=f32)
            mid[:, cols] = (jax.nn.silu(a) * b).astype(bf16)
            return carry

        def down(t, carry):
            cols = pl.ds(pl.multiple_of(t * tile, tile), tile)
            r = jnp.dot(mid[...], w2[:, cols], preferred_element_type=f32).astype(bf16)
            if step == 0:
                back[c, :, cols] = r
            else:
                xs[step, :, cols] = r
            return carry

        lax.fori_loop(0, ffn // ftile, up, 0)
        if step == 7:
            back_forward(1)
        tiles = width // tile
        if step < 4:
            lax.fori_loop(0, tiles, down, 0)
            if step:
                after(step, 0)
        else:
            lax.fori_loop(0, tiles // 2, down, 0)
            after(step, 0)
            lax.fori_loop(tiles // 2, tiles, down, 0)
            after(step, 1)

    for step in range(8):
        if step:
            got_it(xs.at[step], CHUNK + step)
        expert(step)
        if step == 1:
            chunk_forward()
            chunks_sent = len(sent)
        elif step == 6:
            back_forward(0)

    drain(chunks_sent)

    def place(s, k, dst, f):
        ck = code_rows(s)[k:k + 1, :]
        for o in range(SIDE):
            pbuf[o * 2 * cap:(o + 1) * 2 * cap, :] = jnp.where(slots(o) == ck, 1.0, 0.0).astype(bf16)

        def one(t, carry):
            cols = pl.ds(pl.multiple_of(f * wide + t * tile, tile), tile)
            rows = back[:, part(s), cols].reshape(8 * cap, tile)
            dst[:, cols] = lax.dot_general(pbuf[...], rows, (((0,), (0,)), ((), ())), preferred_element_type=f32).astype(bf16)
            return carry

        lax.fori_loop(0, wide // tile, one, 0)

    def unmerged(f):
        h = sides[f]
        for i, (k, o) in enumerate(((0, 1), (1, 3))):
            place(2, k, outq.at[i], f)
            put(outq.at[i, :, h], lbuf.at[i, :, h], HOPP + 2 * f + i, HOPP + 2 * f + i, pdev(o))
        for i, (s, k, o) in enumerate(((3, 1, 1), (1, 0, 3))):
            place(s, k, outq.at[2 + i], f)
            put(outq.at[2 + i, :, h], rbuf.at[1 + i, :, h], HOME + 2 * f + i, HOME + 2 * f + i, pdev(o))

    def mergeable(f):
        place(3, 0, outq.at[4], f)
        place(1, 1, outq.at[5], f)

    def merged(f):
        h = sides[f]
        for i, o in enumerate((1, 3)):
            got_it(lbuf.at[i, :, h], HOPP + 2 * f + i)
            for j, r in enumerate((lo, hi)):
                sid = HOME + 4 + 4 * f + 2 * i + j
                outq[4 + i, r, h] = outq[4 + i, r, h] + lbuf[i, r, h]
                put(outq.at[4 + i, r, h], rbuf.at[3 * i, r, h], sid, sid, pdev(o))

    got_it(back.at[1 - c], BACK + 1 - c)
    for blk in (2, 7):
        got_it(back.at[blk], BACK + blk)
    for f in range(2):
        for blk in (3, 6, 4, 5):
            got_it(back.at[blk, :, sides[f]], BACK + 8 * f + blk)
        unmerged(f)
        if f == 0:
            mergeable(0)
    merged(0)
    mergeable(1)
    merged(1)
    for k in range(2):
        for f in range(2):
            place(0, k, got.at[k], f)
    step_rows = min(64, half)
    for f in range(2):
        h = sides[f]
        for i in range(2):
            got_it(rbuf.at[1 + i, :, h], HOME + 2 * f + i)
        for m, part_rows in enumerate((lo, hi)):
            for i in range(2):
                got_it(rbuf.at[3 * i, part_rows, h], HOME + 4 + 4 * f + 2 * i + m)

            def finish(j, carry):
                r = pl.ds(pl.multiple_of(m * half + j * step_rows, step_rows), step_rows)
                g0, g1 = gate[0, r, 0:1], gate[1, r, 0:1]
                for t in range(wide // tile):
                    cols = pl.ds(f * wide + t * tile, tile)
                    y0 = (got[0, r, cols] + rbuf[0, r, cols] + rbuf[2, r, cols]).astype(f32)
                    y1 = (got[1, r, cols] + rbuf[1, r, cols] + rbuf[3, r, cols]).astype(f32)
                    mixed = g0 * y0 + g1 * y1
                    out[r, cols] = (scale[0] * hid[r, cols].astype(f32) + scale[1] * mixed).astype(bf16)
                return carry

            lax.fori_loop(0, half // step_rows, finish, 0)
    drain()


def fused(hidden, rw, idst, scale, w1, w3, w2, cap):
    tokens, width = hidden.shape
    ffn = w1.shape[1]
    rows = SIDE * cap
    bf = jnp.bfloat16
    hbm = pl.BlockSpec(memory_space=pl.ANY)
    return pl.pallas_call(
        kernel_body,
        out_shape=[
            pltpu.VMEM((tokens, width), bf),
            jax.ShapeDtypeStruct((2, rows, width), bf),
        ],
        in_specs=[hbm, pl.BlockSpec(memory_space=pltpu.SMEM), hbm, hbm, hbm, hbm, hbm],
        out_specs=[pl.BlockSpec(memory_space=pltpu.VMEM), hbm],
        scratch_shapes=[
            pltpu.VMEM(idst.shape, jnp.int32),
            pltpu.VMEM((tokens, width), bf),
            pltpu.VMEM(rw.shape, jnp.float32),
            pltpu.VMEM((width, ffn), bf), pltpu.VMEM((width, ffn), bf), pltpu.VMEM((ffn, width), bf),
            pltpu.VMEM((3, tokens, width), bf),
            pltpu.VMEM((8, tokens), jnp.int32),
            pltpu.VMEM((3, 8, tokens), jnp.int32),
            pltpu.VMEM((2, tokens, 128), jnp.float32),
            pltpu.VMEM((8 * cap, tokens), bf),
            pltpu.VMEM((8, rows, width), bf),
            pltpu.VMEM((7, rows, width), bf),
            pltpu.VMEM((rows, ffn), bf),
            pltpu.VMEM((8, rows, width), bf),
            pltpu.VMEM((2, rows, width), bf),
            pltpu.VMEM((2, tokens, width), bf),
            pltpu.VMEM((4, tokens, width), bf),
            pltpu.SemaphoreType.DMA((NSEND,)),
            pltpu.SemaphoreType.DMA((NMSG,)),
            pltpu.SemaphoreType.DMA((8,)),
        ],
        compiler_params=pltpu.CompilerParams(has_side_effects=True, collective_id=0, vmem_limit_bytes=65800000),
        name='moe',
    )(idst, scale, hidden, rw, w1, w3, w2)[0]


def solution(mesh):
    ep_size = mesh.shape['ep']

    def local_step(hidden, router_w, expert_ids, w_gate, w_up, w_down, post_scale):
        tokens = hidden.shape[0]
        experts = w_gate.shape[0] * ep_size
        cap = tokens // max(1, experts // 8)
        out = fused(hidden, router_w.T, expert_ids.T, post_scale, w_gate[0], w_up[0], w_down[0], cap)
        return out

    tok_spec = P(('dp', 'ep'))
    return jax.shard_map(local_step, mesh=mesh, in_specs=(tok_spec, P(), tok_spec, P('ep'), P('ep'), P('ep'), P()), out_specs=tok_spec, check_vma=False)
```

```python
import functools
import jax
import jax.numpy as jnp
from jax import lax
from jax.experimental import pallas as pl
from jax.experimental.pallas import tpu as pltpu
from jax.sharding import PartitionSpec as P

MESH = pl.DeviceIdType.MESH
SIDE = 4

CODE = 0
GATHER = 3
CHUNK = 9
LEG = 17
BACK = 21
BLEG = 37
HOPP = 41
HOME = 45
NMSG = 57
SFWD = 57
SBFWD = 59
SNBR = 63
SBACK = 67
NSEND = 81
LHID, LRW, LW1, LW3, LW2, LOUT, LIDS = 0, 1, 2, 3, 4, 5, 7


def kernel_body(idsh, scale, hidh, rwh, w1h, w3h, w2h,
                out, fwd, bleg,
                idst, hid, rw, w1, w3, w2, got, code, codes, gate, pbuf, xs, outq, mid, back, lbuf, rbuf,
                send, recv, lsem):
    tokens, width = hid.shape
    cap = xs.shape[1] // SIDE
    ffn = w1.shape[1]
    experts = rw.shape[0]
    half = tokens // 2
    tile = min(512, width // 2)
    wide = width // 2
    sides = (pl.ds(0, wide), pl.ds(wide, wide))
    dtile = min(1024, wide)
    ftile = min(1024, ffn)
    f32, bf16 = jnp.float32, jnp.bfloat16
    me = lax.axis_index('ep')
    y, x, c = lax.div(me, 2 * SIDE), lax.rem(lax.div(me, 2), SIDE), lax.rem(me, 2)

    def dev(yy, xx, cc):
        return (lax.rem(yy, SIDE) * SIDE + lax.rem(xx, SIDE)) * 2 + cc

    def qdev(o, core, axis):
        return dev(y + (1 - axis) * o, x + axis * o, core)

    def pdev(o):
        return dev(y + c * o, x + (1 - c) * o, c)

    def rcopy(src, dst, sid, rid, to):
        return pltpu.make_async_remote_copy(src_ref=src, dst_ref=dst, send_sem=send.at[sid], recv_sem=recv.at[rid], device_id={'ep': to}, device_id_type=MESH)

    sent = []

    def put(src, dst, sid, rid, to):
        cp = rcopy(src, dst, sid, rid, to)
        cp.start()
        sent.append((src, sid))

    def drain(n=None):
        for _ in range(len(sent) if n is None else n):
            src, sid = sent.pop(0)
            rcopy(src, src, sid, 0, me).wait_send()

    def got_it(dst, rid):
        rcopy(dst, dst, 0, rid, me).wait_recv()

    def fetch(src, dst, n):
        cp = pltpu.make_async_copy(src, dst, lsem.at[n])
        cp.start()
        return cp

    lo, hi = pl.ds(0, half), pl.ds(half, half)
    first, last = pl.ds(0, 3 * cap), pl.ds(3 * cap, cap)

    def part(s):
        return pl.ds((0, 1, 3, 2)[s] * cap, cap)

    barrier = pltpu.get_barrier_semaphore()
    peers = [pdev(1), pdev(2), pdev(3), qdev(0, 1 - c, c)]
    peers += [qdev(o, k, c) for o in (1, 3) for k in range(2)]
    peers += [qdev(o, 1 - c, 1 - c) for o in (1, 3)]
    for to in peers:
        pl.semaphore_signal(barrier, inc=1, device_id={'ep': to}, device_id_type=MESH)
    load_hid = fetch(hidh, hid, LHID)
    load_ids = fetch(idsh, idst, LIDS)
    pl.semaphore_wait(barrier, len(peers))

    load_hid.wait()
    put(hid.at[lo], got.at[0, lo], GATHER + 0, GATHER + 0, pdev(1))
    put(hid.at[hi], got.at[2, hi], GATHER + 2, GATHER + 2, pdev(3))
    put(hid.at[hi], got.at[0, hi], GATHER + 1, GATHER + 1, pdev(1))
    put(hid.at[lo], got.at[2, lo], GATHER + 3, GATHER + 3, pdev(3))
    load_rw = fetch(rwh, rw, LRW)
    loads = [fetch(w1h, w1, LW1), fetch(w3h, w3, LW3), fetch(w2h, w2, LW2)]

    load_ids.wait()

    erow = lax.broadcasted_iota(jnp.int32, (experts, tokens), 0)
    hot0, hot1 = idst[0:1, :] == erow, idst[1:2, :] == erow
    one0, one1 = jnp.where(hot0, 1.0, 0.0), jnp.where(hot1, 1.0, 0.0)
    earlier = lax.broadcasted_iota(jnp.int32, (tokens, tokens), 0) < lax.broadcasted_iota(jnp.int32, (tokens, tokens), 1)
    upper = jnp.where(earlier, 1.0, 0.0).astype(bf16)
    before0 = jnp.dot(one0.astype(bf16), upper, preferred_element_type=f32)
    before1 = jnp.dot(one1.astype(bf16), upper, preferred_element_type=f32) + jnp.sum(one0, axis=1, keepdims=True)
    slot0 = jnp.sum(jnp.where(hot0, before0, 0.0), axis=0, keepdims=True)
    slot1 = jnp.sum(jnp.where(hot1, before1, 0.0), axis=0, keepdims=True)
    code[...] = jnp.zeros(code.shape, jnp.int32)
    code[0:1, :] = idst[0:1, :] * cap + slot0.astype(jnp.int32)
    code[1:2, :] = idst[1:2, :] * cap + slot1.astype(jnp.int32)

    order = (2, 1, 3, 0)

    def code_rows(s):
        return code if s == 0 else codes.at[s - 1]

    def slots(o, n=tokens):
        return lax.broadcasted_iota(jnp.int32, (2 * cap, n), 0) + qdev(o, 0, c) * cap

    def pack(s):
        cref = code_rows(s)
        gref = hid if s == 0 else got.at[s - 1]
        c0, c1 = cref[0:1, :], cref[1:2, :]
        for i, o in enumerate(order):
            rows = slots(o)
            pbuf[i * 2 * cap:(i + 1) * 2 * cap, :] = jnp.where((rows == c0) | (rows == c1), 1.0, 0.0).astype(bf16)

        def one(t, carry):
            cols = pl.ds(pl.multiple_of(t * tile, tile), tile)
            r = jnp.dot(pbuf[...], gref[:, cols], preferred_element_type=f32).astype(bf16)
            dst = part(s)
            for i in range(6):
                outq[i, dst, cols] = r[i * cap:(i + 1) * cap]
            r0, r1 = r[6 * cap:7 * cap], r[7 * cap:8 * cap]
            own0 = c == 0
            xs[0, dst, cols] = jnp.where(own0, r0, r1)
            outq[6, dst, cols] = jnp.where(own0, r1, r0)
            return carry

        lax.fori_loop(0, width // tile, one, 0)

    pack(0)
    for s, o in ((1, 1), (3, 3), (2, 2)):
        put(code, codes.at[s - 1], CODE + s - 1, CODE + s - 1, pdev(o))
    got_it(got.at[0, lo], GATHER + 0)
    put(got.at[0, lo], got.at[1, lo], GATHER + 4, GATHER + 4, pdev(1))
    got_it(got.at[2, hi], GATHER + 2)
    put(got.at[2, hi], got.at[1, hi], GATHER + 5, GATHER + 5, pdev(3))

    load_rw.wait()
    w = rw[...]
    wa = w.astype(bf16)
    w = w - wa.astype(f32)
    wb = w.astype(bf16)
    wc = (w - wb.astype(f32)).astype(bf16)
    terms = lax.dot_general(jnp.concatenate([wc, wb, wa], axis=0), hid[...], (((1,), (1,)), ((), ())), preferred_element_type=f32)
    logits = (terms[0:experts] + terms[experts:2 * experts]) + terms[2 * experts:]
    ex = jnp.exp(logits - jnp.max(logits, axis=0, keepdims=True))
    prob = ex / jnp.sum(ex, axis=0, keepdims=True)
    p0 = jnp.sum(jnp.where(hot0, prob, 0.0), axis=0, keepdims=True)
    p1 = jnp.sum(jnp.where(hot1, prob, 0.0), axis=0, keepdims=True)
    gate[0] = jnp.broadcast_to(p0 / (p0 + p1), (128, tokens)).T
    gate[1] = jnp.broadcast_to(p1 / (p0 + p1), (128, tokens)).T

    got_it(codes.at[0], CODE + 0)
    got_it(got.at[0, hi], GATHER + 1)
    pack(1)
    got_it(codes.at[2], CODE + 2)
    got_it(got.at[2, lo], GATHER + 3)
    pack(3)
    put(outq.at[0, first], fwd.at[0, first], LEG + 0, LEG + 0, qdev(1, c, c))
    put(outq.at[1, first], fwd.at[1, first], LEG + 1, LEG + 1, qdev(3, c, c))
    got_it(codes.at[1], CODE + 1)
    got_it(got.at[1, lo], GATHER + 4)
    got_it(got.at[1, hi], GATHER + 5)
    pack(2)

    put(outq.at[0, last], fwd.at[0, last], LEG + 2, LEG + 2, qdev(1, c, c))
    put(outq.at[1, last], fwd.at[1, last], LEG + 3, LEG + 3, qdev(3, c, c))
    put(outq.at[2], xs.at[2 + c], SNBR + 0, CHUNK + 2 + c, qdev(1, 0, c))
    put(outq.at[5], xs.at[2 + c], SNBR + 1, CHUNK + 2 + c, qdev(3, 1, c))
    put(outq.at[6], xs.at[1], CHUNK + 1, CHUNK + 1, qdev(0, 1 - c, c))

    def chunk_forward():
        got_it(fwd.at[0, first], LEG + 0)
        got_it(fwd.at[0, last], LEG + 2)
        put(fwd.at[0], xs.at[4 + c], SFWD + 0, CHUNK + 4 + c, qdev(1, 0, c))
        got_it(fwd.at[1, first], LEG + 1)
        got_it(fwd.at[1, last], LEG + 3)
        put(fwd.at[1], xs.at[4 + c], SFWD + 1, CHUNK + 4 + c, qdev(3, 1, c))
        put(outq.at[3], xs.at[6 + c], SNBR + 2, CHUNK + 6 + c, qdev(1, 1, c))
        put(outq.at[4], xs.at[6 + c], SNBR + 3, CHUNK + 6 + c, qdev(3, 0, c))

    def back_forward(f):
        for i, o in enumerate((1, 3)):
            got_it(bleg.at[i, :, sides[f]], BLEG + 2 * f + i)
            put(bleg.at[i, :, sides[f]], back.at[4 + i, :, sides[f]], SBFWD + 2 * f + i, BACK + 8 * f + 4 + i, qdev(o, c, c))

    def after(step, f):
        k, sid = step % 2, SBACK + 2 * (step - 1)
        if step == 1:
            put(xs.at[1], back.at[c], sid, BACK + c, qdev(0, 1 - c, c))
        elif step in (2, 3):
            put(xs.at[step], back.at[2 + 5 * c], sid, BACK + 2 + 5 * c, qdev(3 + 2 * c, k, k))
        elif step in (4, 5):
            put(xs.at[step, :, sides[f]], bleg.at[c, :, sides[f]], sid + f, BLEG + 2 * f + c, qdev(1 + 2 * c, k, k))
        else:
            put(xs.at[step, :, sides[f]], back.at[6 - 3 * c, :, sides[f]], sid + f, BACK + 8 * f + 6 - 3 * c, qdev(1 + 2 * c, k, k))

    for cp in loads:
        cp.wait()

    def expert(step):
        def up(t, carry):
            cols = pl.ds(pl.multiple_of(t * ftile, ftile), ftile)
            a = jnp.dot(xs[step], w1[:, cols], preferred_element_type=f32)
            b = jnp.dot(xs[step], w3[:, cols], preferred_element_type=f32)
            mid[:, cols] = (jax.nn.silu(a) * b).astype(bf16)
            return carry

        def down(t, carry):
            cols = pl.ds(pl.multiple_of(t * dtile, dtile), dtile)
            r = jnp.dot(mid[...], w2[:, cols], preferred_element_type=f32).astype(bf16)
            if step == 0:
                back[c, :, cols] = r
            else:
                xs[step, :, cols] = r
            return carry

        lax.fori_loop(0, ffn // ftile, up, 0)
        if step == 7:
            back_forward(1)
        tiles = width // dtile
        if step < 4:
            lax.fori_loop(0, tiles, down, 0)
            if step:
                after(step, 0)
        else:
            lax.fori_loop(0, tiles // 2, down, 0)
            after(step, 0)
            lax.fori_loop(tiles // 2, tiles, down, 0)
            after(step, 1)

    for step in range(8):
        if step:
            got_it(xs.at[step], CHUNK + step)
        expert(step)
        if step == 1:
            chunk_forward()
            chunks_sent = len(sent)
        elif step == 6:
            back_forward(0)

    drain(chunks_sent)

    def place(s, k, dst, f):
        ck = code_rows(s)[k:k + 1, :]
        for o in range(SIDE):
            pbuf[o * 2 * cap:(o + 1) * 2 * cap, :] = jnp.where(slots(o) == ck, 1.0, 0.0).astype(bf16)

        def one(t, carry):
            cols = pl.ds(pl.multiple_of(f * wide + t * tile, tile), tile)
            rows = back[:, part(s), cols].reshape(8 * cap, tile)
            dst[:, cols] = lax.dot_general(pbuf[...], rows, (((0,), (0,)), ((), ())), preferred_element_type=f32).astype(bf16)
            return carry

        lax.fori_loop(0, wide // tile, one, 0)

    def unmerged(f):
        h = sides[f]
        for i, (k, o) in enumerate(((0, 1), (1, 3))):
            place(2, k, outq.at[i], f)
            put(outq.at[i, :, h], lbuf.at[i, :, h], HOPP + 2 * f + i, HOPP + 2 * f + i, pdev(o))
        for i, (s, k, o) in enumerate(((3, 1, 1), (1, 0, 3))):
            place(s, k, outq.at[2 + i], f)
            put(outq.at[2 + i, :, h], rbuf.at[1 + i, :, h], HOME + 2 * f + i, HOME + 2 * f + i, pdev(o))

    def mergeable(f):
        place(3, 0, outq.at[4], f)
        place(1, 1, outq.at[5], f)

    def merged(f):
        h = sides[f]
        for i, o in enumerate((1, 3)):
            got_it(lbuf.at[i, :, h], HOPP + 2 * f + i)
            for j, r in enumerate((lo, hi)):
                sid = HOME + 4 + 4 * f + 2 * i + j
                outq[4 + i, r, h] = outq[4 + i, r, h] + lbuf[i, r, h]
                put(outq.at[4 + i, r, h], rbuf.at[3 * i, r, h], sid, sid, pdev(o))

    got_it(back.at[1 - c], BACK + 1 - c)
    for blk in (2, 7):
        got_it(back.at[blk], BACK + blk)
    for f in range(2):
        for blk in (3, 6, 4, 5):
            got_it(back.at[blk, :, sides[f]], BACK + 8 * f + blk)
        unmerged(f)
        if f == 0:
            mergeable(0)
    merged(0)
    mergeable(1)
    merged(1)
    for k in range(2):
        for f in range(2):
            place(0, k, got.at[k], f)
    step_rows = min(64, half)
    for f in range(2):
        h = sides[f]
        for i in range(2):
            got_it(rbuf.at[1 + i, :, h], HOME + 2 * f + i)
        for m, part_rows in enumerate((lo, hi)):
            for i in range(2):
                got_it(rbuf.at[3 * i, part_rows, h], HOME + 4 + 4 * f + 2 * i + m)

            def finish(j, carry):
                r = pl.ds(pl.multiple_of(m * half + j * step_rows, step_rows), step_rows)
                g0, g1 = gate[0, r, 0:1], gate[1, r, 0:1]
                for t in range(wide // tile):
                    cols = pl.ds(f * wide + t * tile, tile)
                    y0 = (got[0, r, cols] + rbuf[0, r, cols] + rbuf[2, r, cols]).astype(f32)
                    y1 = (got[1, r, cols] + rbuf[1, r, cols] + rbuf[3, r, cols]).astype(f32)
                    mixed = g0 * y0 + g1 * y1
                    out[r, cols] = (scale[0] * hid[r, cols].astype(f32) + scale[1] * mixed).astype(bf16)
                return carry

            lax.fori_loop(0, half // step_rows, finish, 0)
    drain()


def fused(hidden, rw, idst, scale, w1, w3, w2, cap):
    tokens, width = hidden.shape
    ffn = w1.shape[1]
    rows = SIDE * cap
    bf = jnp.bfloat16
    hbm = pl.BlockSpec(memory_space=pl.ANY)
    return pl.pallas_call(
        kernel_body,
        out_shape=[
            pltpu.VMEM((tokens, width), bf),
            jax.ShapeDtypeStruct((2, rows, width), bf),
            jax.ShapeDtypeStruct((2, rows, width), bf),
        ],
        in_specs=[hbm, pl.BlockSpec(memory_space=pltpu.SMEM), hbm, hbm, hbm, hbm, hbm],
        out_specs=[pl.BlockSpec(memory_space=pltpu.VMEM), hbm, hbm],
        scratch_shapes=[
            pltpu.VMEM(idst.shape, jnp.int32),
            pltpu.VMEM((tokens, width), bf),
            pltpu.VMEM(rw.shape, jnp.float32),
            pltpu.VMEM((width, ffn), bf), pltpu.VMEM((width, ffn), bf), pltpu.VMEM((ffn, width), bf),
            pltpu.VMEM((3, tokens, width), bf),
            pltpu.VMEM((8, tokens), jnp.int32),
            pltpu.VMEM((3, 8, tokens), jnp.int32),
            pltpu.VMEM((2, tokens, 128), jnp.float32),
            pltpu.VMEM((8 * cap, tokens), bf),
            pltpu.VMEM((8, rows, width), bf),
            pltpu.VMEM((7, rows, width), bf),
            pltpu.VMEM((rows, ffn), bf),
            pltpu.VMEM((8, rows, width), bf),
            pltpu.VMEM((2, tokens, width), bf),
            pltpu.VMEM((4, tokens, width), bf),
            pltpu.SemaphoreType.DMA((NSEND,)),
            pltpu.SemaphoreType.DMA((NMSG,)),
            pltpu.SemaphoreType.DMA((8,)),
        ],
        compiler_params=pltpu.CompilerParams(has_side_effects=True, collective_id=0, vmem_limit_bytes=65500000),
        name='moe',
    )(idst, scale, hidden, rw, w1, w3, w2)[0]


def solution(mesh):
    ep_size = mesh.shape['ep']

    def local_step(hidden, router_w, expert_ids, w_gate, w_up, w_down, post_scale):
        tokens = hidden.shape[0]
        experts = w_gate.shape[0] * ep_size
        cap = tokens // max(1, experts // 8)
        out = fused(hidden, router_w.T, expert_ids.T, post_scale, w_gate[0], w_up[0], w_down[0], cap)
        return out

    tok_spec = P(('dp', 'ep'))
    return jax.shard_map(local_step, mesh=mesh, in_specs=(tok_spec, P(), tok_spec, P('ep'), P('ep'), P('ep'), P()), out_specs=tok_spec, check_vma=False)
```
